32 devices in a mesh: gx: 4 (over y, x), gy: 4 (over z), gz: 2 (over core).
Axes of the slice: x: 2, y: 2, z: 4, core: 2. Of those that a mesh axis runs over, the one named last changes fastest.
Arguments:
- estimate: float32 [16, 256, 512], P('gz', 'gx', 'gy'), may hold values from 0.25 to 4
- view_data: float32 [16, 256, 512], P('gz', 'gx', 'gy'), may hold values from 0.25 to 4
- psf_stack: float32 [6, 31, 31, 31], replicated, may hold values from 0.01 to 1.53, as said below
- view_index: int32 [1], replicated, may hold values from 0 to 5
Outputs:
- updated_estimate: float32 [16, 256, 512], P('gz', 'gx', 'gy')
- level_one: float32 [8, 128, 256], P('gz', 'gx', 'gy')
- level_two: float32 [4, 64, 128], P('gz', 'gx', 'gy')
- level_three: float32 [2, 32, 64], P('gz', 'gx', 'gy')
- level_four: float32 [1, 16, 32], P(None, 'gx', 'gy')
- level_five: float32 [1, 8, 16], replicated
The draws below stay inside these ranges and needn't reach their ends.
Inputs may be any that keep to these rules, and one draw needn't show every extreme that they name: `psf_stack`: every entry of every view's point spread function is positive.
All inputs are finite; a program needn't handle non-finite values.
Results may differ from the reference program's by a relative error of at most 0.000075.
Values sent between devices are 32-bit elements; how exact they have to be, the bound alone decides.
A program may use at most 128 MiB of HBM per device.

```python
import math
import jax
import jax.numpy as jnp
from jax import lax

HALO = 15
VIEWS = 6
NX = 256
NY = 512
NZ = 16


def draw_psf_stack(key, part):
    extent = 2 * HALO + 1
    first, second, third = jax.random.split(jax.random.fold_in(key, 7), 3)
    widths = jax.random.uniform(first, (VIEWS, 3), jnp.float32, 1.0, 4.5)
    offsets = jnp.arange(extent, dtype=jnp.float32) - HALO
    depth_term = offsets[None, :, None, None] / widths[:, 0, None, None, None]
    row_term = offsets[None, None, :, None] / widths[:, 1, None, None, None]
    column_term = offsets[None, None, None, :] / widths[:, 2, None, None, None]
    exponent = depth_term * depth_term + row_term * row_term + column_term * column_term
    roughness = jax.random.uniform(second, (VIEWS, extent, extent, extent), jnp.float32, 0.5, 1.5)
    floor_part = 0.02 * jax.random.uniform(third, (VIEWS, extent, extent, extent), jnp.float32, 0.5, 1.5)
    return jnp.exp(-0.5 * exponent) * roughness + floor_part


def levels(own_key, shape, cuts, least, high):
    def one(position, parts):
        steps = jax.random.uniform(jax.random.fold_in(jax.random.fold_in(own_key, 6), position), (parts,), jnp.float32, least / len(cuts), high / len(cuts))
        return jnp.repeat(jnp.exp(steps), shape[position] // parts).reshape((-1,) + (1,) * (len(shape) - position - 1))

    loudness = one(*cuts[0])
    for cut in cuts[1:]:
        loudness = loudness * one(*cut)
    return loudness


def setup_inputs(seed: int = 0) -> dict:
    streams_of = jax.random.split(jax.random.key(seed), 5)
    return {
        "estimate": jnp.clip(jnp.exp(math.log(4.0) - 2.7725887 * jax.random.uniform(streams_of[0], (NZ, NX, NY), jnp.float32) ** levels(streams_of[0], (NZ, NX, NY), ((0, 2), (1, 4), (2, 4)), -0.2, 0.2)), 0.25, 4.0),
        "view_data": jnp.clip(jnp.exp(math.log(4.0) - 2.7725887 * jax.random.uniform(streams_of[1], (NZ, NX, NY), jnp.float32) ** levels(streams_of[1], (NZ, NX, NY), ((0, 2), (1, 4), (2, 4)), -0.2, 0.2)), 0.25, 4.0),
        "psf_stack": draw_psf_stack(jax.random.fold_in(streams_of[4], 71), 0),
        "view_index": jax.random.randint(streams_of[3], (1,), 0, VIEWS).astype(jnp.int32),
    }


def convolve(volume, kernel):
    radius = (kernel.shape[0] - 1) // 2
    fft_sizes = tuple(((extent + 2 * radius + 15) // 16) * 16 for extent in volume.shape)
    product = jnp.fft.rfftn(volume, fft_sizes) * jnp.fft.rfftn(kernel, fft_sizes)
    full_conv = jnp.fft.irfftn(product, fft_sizes)
    plane_count, row_count, column_count = volume.shape
    return full_conv[radius:radius + plane_count, radius:radius + row_count, radius:radius + column_count].astype(jnp.float32)


def average_blocks(volume, depth):
    plane_count, row_count, column_count = volume.shape
    if depth:
        blocks = volume.reshape(plane_count // 2, 2, row_count // 2, 2, column_count // 2, 2)
        return jnp.mean(blocks, axis=(1, 3, 5))
    blocks = volume.reshape(plane_count, row_count // 2, 2, column_count // 2, 2)
    return jnp.mean(blocks, axis=(2, 4))


def reference(estimate, view_data, psf_stack, view_index):
    kernel = lax.dynamic_index_in_dim(psf_stack, view_index[0], 0, keepdims=False)
    kernel = kernel / jnp.sum(kernel)
    blurred = convolve(estimate, kernel)
    ratio_field = view_data / blurred
    correction = convolve(ratio_field, jnp.flip(kernel))
    updated = estimate * correction
    level_one = average_blocks(updated, True)
    level_two = average_blocks(level_one, True)
    level_three = average_blocks(level_two, True)
    level_four = average_blocks(level_three, True)
    level_five = average_blocks(level_four, False)
    return updated, level_one, level_two, level_three, level_four, level_five
```

```python
import functools
import math

import jax
import jax.numpy as jnp
import numpy as np
from jax import lax
from jax.experimental import pallas as pl
from jax.experimental.pallas import tpu as pltpu
from jax.sharding import PartitionSpec as P

MESH = pl.DeviceIdType.MESH
NS = jax.named_scope
BF = jnp.bfloat16
F32 = jnp.float32
LANES = 128
EDGE = 16
GROUP = 8
CORNERS = ((1, 1), (-1, 1), (1, -1), (-1, -1))
SIDES_X = ((1, 0), (-1, 0))
SIDES_Y = ((0, 1), (0, -1))


def two_parts(matrix):
    matrix = np.asarray(matrix, np.float32)
    high = matrix.astype(BF)
    low = (matrix - high.astype(np.float32)).astype(BF)
    return high, low


def split(x):
    high = x.astype(BF)
    return high, (x - high.astype(F32)).astype(BF)


def dot(a, b):
    return jnp.dot(a, b, preferred_element_type=F32)


def tables(nx, ny, extent):
    radius = (extent - 1) // 2
    lx, ly = nx + 2 * EDGE, ny + 2 * EDGE
    nf = ly // 2 + 1
    wide = extent + 1
    freq_y = np.arange(nf)
    freq_x = np.arange(lx)

    def wave(k, n, length):
        return 2 * math.pi / length * np.mod(np.outer(k, n), length)

    pos = np.concatenate([EDGE + np.arange(ny), np.arange(EDGE), EDGE + ny + np.arange(EDGE)])
    fy = np.zeros((ny + 2 * EDGE, 2 * LANES))
    angle = wave(pos, freq_y, ly)
    fy[:, :nf] = np.cos(angle)
    fy[:, LANES : LANES + nf] = -np.sin(angle)
    ky = np.zeros((wide, 2 * LANES))
    angle = wave(np.arange(extent) - radius, freq_y, ly)
    ky[:extent, :nf] = np.cos(angle)
    ky[:extent, LANES : LANES + nf] = -np.sin(angle)
    iy = np.zeros((2 * LANES, ny))
    weight = np.full((nf, 1), 2.0)
    weight[0] = weight[-1] = 1.0
    angle = wave(freq_y, EDGE + np.arange(ny), ly)
    iy[:nf] = weight / ly * np.cos(angle)
    iy[LANES : LANES + nf] = -weight / ly * np.sin(angle)

    angle = wave(freq_x, np.arange(lx), lx)
    fx = np.block([[np.cos(angle), np.sin(angle)], [-np.sin(angle), np.cos(angle)]])
    angle = wave(EDGE + np.arange(nx), freq_x, lx)
    ix = np.block([[np.cos(angle), -np.sin(angle)], [np.sin(angle), np.cos(angle)]]) / lx
    kx = np.zeros((2 * lx, 2, wide))
    angle = wave(freq_x, np.arange(extent) - radius, lx)
    kx[:lx, 0, :extent] = np.cos(angle)
    kx[:lx, 1, :extent] = np.sin(angle)
    kx[lx:, 0, :extent] = -np.sin(angle)
    kx[lx:, 1, :extent] = np.cos(angle)
    kx = kx.reshape(2 * lx, 2 * wide)

    fy_hi, fy_lo = two_parts(fy)
    ky_hi, ky_lo = two_parts(ky)
    iy_hi, iy_lo = two_parts(iy)
    fx_hi, fx_lo = two_parts(fx)
    ix_hi, ix_lo = two_parts(ix)
    kx_hi, kx_lo = two_parts(kx)

    py = np.zeros((ny, LANES))
    px = np.zeros((nx, nx))
    row, col = 0, 0
    places = []
    for level in range(1, 5):
        size = 2**level
        rows, cols = nx // size, ny // size
        places.append((row, rows, col, cols))
        for r in range(rows):
            px[row + r, r * size : (r + 1) * size] = 1.0 / size
        for c in range(cols):
            py[c * size : (c + 1) * size, col + c] = 1.0 / size
        row, col = row + rows, col + cols

    blank = np.zeros((LANES - 3 * wide, 2 * LANES), BF)
    side_hi, side_lo = fy_hi[ny:], fy_lo[ny:]
    named = {
        "fya": np.concatenate([fy_hi[:ny], fy_hi[:ny]], 0),
        "fyb": np.concatenate([fy_lo[:ny], side_hi, side_hi, side_lo, blank], 0),
        "fx2": np.concatenate([fx_hi, fx_lo], 0),
        "ky3": np.concatenate([ky_hi, ky_hi, ky_lo, blank], 0),
        "kx3": np.concatenate([kx_hi, kx_hi, kx_lo], 1),
        "ix2": np.concatenate([ix_hi, ix_lo], 0),
        "iyh": iy_hi,
        "iyl": iy_lo,
        "py": py.astype(BF),
        "px": px.astype(BF),
    }
    stacked, where, row = [], {}, 0
    for name, a in named.items():
        rows, cols = a.shape
        where[name] = (row, rows, cols)
        full = np.zeros((rows, 2 * LANES), BF)
        full[:, :cols] = a
        stacked.append(full)
        row += rows
    return np.concatenate(stacked, 0), where, tuple(places)


def kernel(
    sizes, where, places,
    index_hbm, est_hbm, view_hbm, psf_hbm, table_hbm,
    out_ref, one_ref, two_ref, three_ref, four_ref, five_ref,
    index_ref, est_ref, view_ref, psf, table,
    psf_pad, k2, own, peer, mix, ratio,
    pack, xhalo, yhalo, share, share_in, place5, mine, tiles, ruler,
    in_sem, hs, hr, es, er, ps, pr, gs, gr,
):
    gxn, gyn = sizes
    nz, nx, ny = est_ref.shape
    extent = psf.shape[1]
    wide = extent + 1
    pairs = nz // 2
    lx = nx + 2 * EDGE
    nf = (ny + 2 * EDGE) // 2 + 1
    third = lx // 3
    lp = 2 * third
    half = (nf + 1) // 2
    middle = (extent - 1) // 2
    gx, gy, gz = lax.axis_index("gx"), lax.axis_index("gy"), lax.axis_index("gz")
    partner = {"gx": gx, "gy": gy, "gz": 1 - gz}
    chips = gxn * gyn
    everyone = 2 * chips

    def tab(name, first=0, count=None):
        row, rows, cols = where[name]
        return table[pl.ds(row + first, rows if count is None else count), pl.ds(0, cols)]

    load_est, load_index, load_psf, load_table, load_view = [
        pltpu.make_async_copy(a, b, in_sem.at[i])
        for i, (a, b) in enumerate(
            (
                (est_hbm, est_ref),
                (index_hbm, index_ref),
                (psf_hbm, psf),
                (table_hbm, table),
                (view_hbm, view_ref),
            )
        )
    ]
    load_est.start()

    def device_at(offset):
        chip = offset // 2
        x = lax.rem(gx + chip // gyn, gxn)
        y = lax.rem(gy + lax.rem(chip, gyn), gyn)
        return {"gx": x, "gy": y, "gz": lax.rem(gz + lax.rem(offset, 2), 2)}

    barrier = pltpu.get_barrier_semaphore()

    @pl.loop(1, everyone)
    def _(offset):
        pl.semaphore_signal(barrier, inc=1, device_id=device_at(offset), device_id_type=MESH)

    load_psf.start()
    load_index.start()
    load_table.start()
    load_view.start()

    def exists(dx, dy):
        ok = None
        for c, n, d in ((gx, gxn, dx), (gy, gyn, dy)):
            if d > 0:
                t = c < n - 1
            elif d < 0:
                t = c > 0
            else:
                continue
            ok = t if ok is None else jnp.logical_and(ok, t)
        return ok

    def halo_copy(phase, field, dx, dy, planes=None):
        if dy == 0:
            rows = slice(nx - EDGE, nx) if dx > 0 else slice(0, EDGE)
            source = field.at[planes, rows, :]
            target = xhalo.at[phase, 0 if dx > 0 else 1, planes]
        else:
            side = 0 if dy > 0 else 1
            if dx == 0:
                source, target = pack.at[phase, side], yhalo.at[phase, side, pl.ds(EDGE, nx), :]
            else:
                rows = pl.ds(nx - EDGE, EDGE) if dx > 0 else pl.ds(0, EDGE)
                to = pl.ds(0, EDGE) if dx > 0 else pl.ds(EDGE + nx, EDGE)
                source, target = pack.at[phase, side, rows, :], yhalo.at[phase, side, to, :]
        return pltpu.make_async_remote_copy(
            src_ref=source,
            dst_ref=target,
            send_sem=hs.at[phase],
            recv_sem=hr.at[phase],
            device_id={"gx": gx + dx, "gy": gy + dy, "gz": gz},
            device_id_type=MESH,
        )

    def send_halo(phase, field, directions, planes=None):
        for dx, dy in directions:

            @pl.when(exists(dx, dy))
            def _():
                halo_copy(phase, field, dx, dy, planes).start()

    beside_x = (gx > 0).astype(jnp.int32) + (gx < gxn - 1).astype(jnp.int32)
    beside_y = (gy > 0).astype(jnp.int32) + (gy < gyn - 1).astype(jnp.int32)

    def settle(sem):
        for a in range(3):
            for b in range(3):
                rows = nz * EDGE * a + nx * b + EDGE * a * b
                if rows:

                    @pl.when(jnp.logical_and(beside_x == a, beside_y == b))
                    def _():
                        part = ruler.at[pl.ds(0, rows)]
                        pltpu.make_async_copy(part, part, sem).wait()

    def add_to_pack(phase, z, plane, first):
        lane = lax.broadcasted_iota(jnp.int32, (nx, LANES), 1) // EDGE
        for side, shift in ((0, EDGE * z + EDGE), (1, EDGE * z)):
            moved = pltpu.roll(plane, shift % LANES, 1) if shift % LANES else plane
            kept = 0.0 if first else pack[phase, side]
            pack[phase, side] = jnp.where(lane == z, moved, kept)

    def zero_missing(phase):
        for dx, dy in SIDES_X + SIDES_Y + CORNERS:
            if dy == 0:
                target = xhalo.at[phase, 0 if dx > 0 else 1]
            else:
                side = 0 if dy > 0 else 1
                first, count = {0: (EDGE, nx), 1: (0, EDGE), -1: (EDGE + nx, EDGE)}[dx]
                target = yhalo.at[phase, side, pl.ds(first, count), :]

            @pl.when(jnp.logical_not(exists(-dx, -dy)))
            def _():
                target[...] = jnp.zeros(target.shape, F32)

    def swap_copy(phase, first, count):
        planes = pl.ds(first, count)
        return pltpu.make_async_remote_copy(
            src_ref=own.at[phase, planes],
            dst_ref=peer.at[phase, planes],
            send_sem=es.at[phase],
            recv_sem=er.at[phase],
            device_id=partner,
            device_id_type=MESH,
        )

    def fold(x):
        lane = lax.broadcasted_iota(jnp.int32, (lp, LANES), 1)
        rest = x[lp:lx]
        beside = jnp.concatenate(
            [pltpu.roll(rest, nf, 1), pltpu.roll(rest, nf - half, 1)], axis=0
        )
        return jnp.where(lane < nf, x[:lp], beside)

    def unfold(x):
        lane = lax.broadcasted_iota(jnp.int32, (third, LANES), 1)
        low = pltpu.roll(x[:third], LANES - nf, 1)
        high = pltpu.roll(x[third:lp], LANES - (nf - half), 1)
        return jnp.concatenate([x[:lp], jnp.where(lane < half, low, high)], axis=0)

    def forward(phase, field, q):
        lane = lax.broadcasted_iota(jnp.int32, (lx, LANES), 1)
        rows, sides = [], []
        for z in (2 * q, 2 * q + 1):
            rows.append(xhalo[phase, 0, z])
            rows.append(field[z])
            rows.append(xhalo[phase, 1, z])
            left, right = yhalo[phase, 0], yhalo[phase, 1]
            if z:
                left = pltpu.roll(left, LANES - EDGE * z, 1)
            if z != 1:
                right = pltpu.roll(right, (EDGE - EDGE * z) % LANES, 1)
            side = jnp.where(lane < EDGE, left, jnp.where(lane < 2 * EDGE, right, 0.0))
            high = side.astype(BF).astype(F32)
            low = side - high
            sides.append(
                (high + pltpu.roll(low, 2 * EDGE, 1) + pltpu.roll(high, 4 * EDGE, 1)).astype(BF)
            )
        hi, lo = split(jnp.concatenate(rows, axis=0))
        x1 = dot(jnp.concatenate([hi, lo], axis=1), tab("fya")) + dot(
            jnp.concatenate([hi, jnp.concatenate(sides, axis=0)], axis=1), tab("fyb")
        )
        stacked = [
            jnp.concatenate(
                [x1[k * lx : (k + 1) * lx, :LANES], x1[k * lx : (k + 1) * lx, LANES:]], axis=0
            )
            for k in range(2)
        ]
        hi, lo = split(jnp.concatenate(stacked, axis=1))
        both = dot(tab("fx2"), hi)
        x2 = both[: 2 * lx] + both[2 * lx :] + dot(tab("fx2", 0, 2 * lx), lo)
        for k in range(2):
            part = x2[:, k * LANES : (k + 1) * LANES]
            own[phase, 2 * q + k, pl.ds(0, lp), :] = fold(part[:lx])
            own[phase, 2 * q + k, pl.ds(lp, lp), :] = fold(part[lx:])

    def mix_planes(source, phase, base, conj, add, chosen):
        @pl.loop(0, lp // 8)
        def _(s):
            re = pl.ds(pl.multiple_of(s * 8, 8), 8)
            im = pl.ds(pl.multiple_of(lp + s * 8, 8), 8)
            vr = [source[phase, j, re, :] for j in range(nz)]
            vi = [source[phase, j, im, :] for j in range(nz)]
            kr, ki = {}, {}
            reach = [(j - i if conj else i - j) for i in chosen for j in range(nz)]
            for d in sorted(set(reach)):
                kr[d] = k2[base + d, re, :]
                ki[d] = k2[base + d, im, :]
            ks = {d: kr[d] - ki[d] if conj else kr[d] + ki[d] for d in kr}
            vs = [r + i for r, i in zip(vr, vi)]
            for i in chosen:
                a = b = c = None
                for j in range(nz):
                    d = j - i if conj else i - j
                    rr, ii, ss = kr[d] * vr[j], ki[d] * vi[j], ks[d] * vs[j]
                    a = rr if a is None else a + rr
                    b = ii if b is None else b + ii
                    c = ss if c is None else c + ss
                yr = a + b if conj else a - b
                yi = c - a + b if conj else c - a - b
                mix[i, re, :] = mix[i, re, :] + yr if add else yr
                mix[i, im, :] = mix[i, im, :] + yi if add else yi

    def inverse(planes, write):
        for z in planes:
            y = jnp.concatenate(
                [
                    jnp.concatenate([unfold(mix[w, pl.ds(0, lp)]), unfold(mix[w, pl.ds(lp, lp)])], 0)
                    for w in (z, z + 1)
                ],
                axis=1,
            )
            hi, lo = split(y)
            both = dot(tab("ix2"), hi)
            g = both[: 2 * nx] + both[2 * nx :] + dot(tab("ix2", 0, 2 * nx), lo)
            for k in range(2):
                part = g[:, k * LANES : (k + 1) * LANES]
                rows = jnp.concatenate([part[:nx], part[nx:]], axis=1)
                hi, lo = split(rows)
                write(z + k, dot(hi, tab("iyh")) + dot(lo, tab("iyh")) + dot(hi, tab("iyl")))

    def prepare(first):
        block = psf_pad[pl.ds(first, GROUP)].reshape(GROUP * wide, LANES)
        high = block.astype(BF).astype(F32)
        low = block - high
        x1 = dot(
            (high + pltpu.roll(low, wide, 1) + pltpu.roll(high, 2 * wide, 1)).astype(BF),
            tab("ky3"),
        )
        hi, lo = split(x1)
        hi = hi.reshape(GROUP, wide, 2 * LANES)
        lo = lo.reshape(GROUP, wide, 2 * LANES)
        for h in range(GROUP // 2):
            columns = []
            for n in (2 * h, 2 * h + 1):
                parts = []
                for part in (hi[n], lo[n], hi[n]):
                    parts.append(part[:, :LANES])
                    parts.append(part[:, LANES:])
                columns.append(jnp.concatenate(parts, axis=0))
            spectrum = dot(tab("kx3"), jnp.concatenate(columns, axis=1))
            for n in range(2):
                part = spectrum[:, n * LANES : (n + 1) * LANES]
                k2[first + 2 * h + n, pl.ds(0, lp), :] = fold(part[:lx])
                k2[first + 2 * h + n, pl.ds(lp, lp), :] = fold(part[lx:])

    def convolve(phase, field, conj, groups, write, after):
        with NS(f"wait_halo{phase}"):
            settle(hr.at[phase])
        count = nz // 2
        for n in range(2):
            with NS(f"forward{phase}_{n}"):
                for q in range(n * pairs // 2, (n + 1) * pairs // 2):
                    forward(phase, field, q)
                swap_copy(phase, n * count, count).start()
        sign = 1 - 2 * gz if conj else 2 * gz - 1
        with NS(f"mixown{phase}"):
            mix_planes(own, phase, middle, conj, False, range(nz))
        if phase == 0:
            with NS("prepare2"):
                prepare(3 * GROUP * gz)
        with NS(f"waitswap{phase}"):
            pltpu.make_async_copy(own.at[phase], peer.at[phase], er.at[phase]).wait()
        size = nz // groups
        for n in range(groups):
            planes = range(n * size, (n + 1) * size)
            with NS(f"mixpeer{phase}_{n}"):
                mix_planes(peer, phase, middle + sign * nz, conj, True, planes)
            with NS(f"inverse{phase}_{n}"):
                inverse(planes[::2], write)
                after(planes)

    with NS("zero"):
        zero_missing(0)
        zero_missing(1)
    with NS("wait_est"):
        load_est.wait()
    with NS("pack0"):
        for z in range(nz):
            add_to_pack(0, z, est_ref[z], z == 0)
    with NS("barrier"):
        pl.semaphore_wait(barrier, everyone - 1)
    with NS("send0"):
        send_halo(0, est_ref, CORNERS)
        send_halo(0, est_ref, SIDES_X, pl.ds(0, nz))
        send_halo(0, est_ref, SIDES_Y)

    with NS("wait_loads"):
        load_index.wait()
        load_psf.wait()
        load_table.wait()
        load_view.wait()
    with NS("psf_prep"):
        chosen = psf[index_ref[0]]
        total = jnp.sum(chosen, axis=0)
        total = jnp.sum(jnp.sum(total, axis=1, keepdims=True), axis=0, keepdims=True)
        psf_pad[...] = jnp.zeros(psf_pad.shape, F32)
        psf_pad[pl.ds(0, extent), pl.ds(0, extent), pl.ds(0, extent)] = (
            chosen * (1.0 / total)[None]
        )

    with NS("prepare1"):

        @pl.loop(1, 3)
        def _(g):
            prepare(g * GROUP)

    def write_ratio(z, blurred):
        value = view_ref[z] / blurred
        ratio[z] = value
        add_to_pack(1, z, value, z == 0)

    def after_ratio(planes):
        if planes[-1] == nz - 1:
            send_halo(1, ratio, CORNERS)
        send_halo(1, ratio, SIDES_X, pl.ds(planes[0], len(planes)))
        if planes[-1] == nz - 1:
            send_halo(1, ratio, SIDES_Y)

    convolve(0, est_ref, False, 2, write_ratio, after_ratio)

    with NS("prepare3"):
        prepare(3 * GROUP * (1 - gz))
        cols5 = four_ref.shape[2] // 2
        i = lax.broadcasted_iota(jnp.int32, (LANES, LANES), 0)
        j = lax.broadcasted_iota(jnp.int32, (LANES, LANES), 1)
        target = i // (ny // cols5) + gy * cols5
        place5[...] = jnp.where(j == target, 1.0 / (nz * 2 * 32 * 32), 0.0).astype(BF)

    def write_update(z, correction):
        out_ref[z] = est_ref[z] * correction

    convolve(1, ratio, True, 1, write_update, lambda planes: None)

    with NS("five_send"):
        rows5 = four_ref.shape[1] // 2
        total = out_ref[0]
        for z in range(1, nz):
            total = total + out_ref[z]
        summed = jnp.sum(total.reshape(rows5, nx // rows5, ny), axis=1)
        hi, lo = split(summed)
        mine[...] = dot(hi, place5[...]) + dot(lo, place5[...])

        def slot(x, y, z):
            return (x * gyn + y) * 2 + z

        def tile_copy(offset):
            return pltpu.make_async_remote_copy(
                src_ref=mine,
                dst_ref=tiles.at[slot(gx, gy, gz)],
                send_sem=gs,
                recv_sem=gr,
                device_id=device_at(offset),
                device_id_type=MESH,
            )

        @pl.loop(1, everyone)
        def _(offset):
            tile_copy(offset).start()

        tiles[slot(gx, gy, gz)] = mine[...]

    def pooled(plane):
        hi, lo = split(plane)
        t = dot(hi, tab("py")) + dot(lo, tab("py"))
        hi, lo = split(t)
        return dot(tab("px"), hi) + dot(tab("px"), lo)

    with NS("pyramid"):
        halves = [(out_ref[2 * i] + out_ref[2 * i + 1]) * 0.5 for i in range(nz // 2)]
        quarters = [(halves[2 * i] + halves[2 * i + 1]) * 0.5 for i in range(nz // 4)]
        eighth = (quarters[0] + quarters[1]) * 0.5
        r4, c4 = places[3][0], places[3][2]
        last = pooled(eighth)
        share[0] = last[r4 : r4 + 8]
        share_copy = pltpu.make_async_remote_copy(
            src_ref=share.at[0], dst_ref=share_in, send_sem=ps, recv_sem=pr,
            device_id=partner, device_id_type=MESH,
        )
        share_copy.start()
        row, rows, col, cols = places[2]
        three_ref[0] = last[row : row + rows, col : col + cols]
        row, rows, col, cols = places[1]
        for i, plane in enumerate(quarters):
            two_ref[i] = pooled(plane)[row : row + rows, col : col + cols]
        row, rows, col, cols = places[0]
        for i, plane in enumerate(halves):
            one_ref[i] = pooled(plane)[row : row + rows, col : col + cols]
    with NS("share"):
        share_copy.wait()
        both = (share[0] + share_in[...]) * 0.5
        four_ref[0] = both[: places[3][1], c4 : c4 + places[3][3]]
    with NS("settle"):
        for phase in range(2):
            settle(hs.at[phase])
            pltpu.make_async_copy(own.at[phase], peer.at[phase], es.at[phase]).wait()
    with NS("wait_tiles"):
        others = tiles.at[pl.ds(0, everyone - 1)]
        pltpu.make_async_copy(others, others, gs).wait()
        pltpu.make_async_copy(others, others, gr).wait()
    with NS("five"):
        for x in range(gxn):
            five = tiles[slot(x, 0, 0)]
            for n in range(1, 2 * gyn):
                five = five + tiles[slot(x, 0, 0) + n]
            five_ref[0, pl.ds(x * rows5, rows5), :] = five[:, : five_ref.shape[2]]


def write_out(*refs):
    sems = refs[12]
    copies = [pltpu.make_async_copy(refs[i], refs[6 + i], sems.at[i]) for i in range(6)]
    for copy in copies:
        copy.start()
    for copy in copies:
        copy.wait()


def local(sizes, estimate, view_data, psf_stack, view_index):
    gxn, gyn = sizes
    nz, nx, ny = estimate.shape
    extent = psf_stack.shape[1]
    table, where, places = tables(nx, ny, extent)
    lx = nx + 2 * EDGE
    lp = 2 * (lx // 3)
    wide = extent + 1
    everyone = 2 * gxn * gyn
    vmem = pl.BlockSpec(memory_space=pltpu.VMEM)
    hbm = pl.BlockSpec(memory_space=pltpu.HBM)
    rows5, cols5 = nx // 32, ny // 32
    dma = pltpu.SemaphoreType.DMA
    shapes = (
        (nz, nx, ny),
        (nz // 2, nx // 2, ny // 2),
        (nz // 4, nx // 4, ny // 4),
        (nz // 8, nx // 8, ny // 8),
        (1, nx // 16, ny // 16),
        (1, rows5 * gxn, cols5 * gyn),
    )
    results = pl.pallas_call(
        functools.partial(kernel, sizes, where, places),
        out_shape=tuple(pltpu.VMEM(s, F32) for s in shapes),
        in_specs=[hbm] * 5,
        out_specs=(vmem,) * 6,
        scratch_shapes=[
            pltpu.SMEM(view_index.shape, view_index.dtype),
            pltpu.VMEM(estimate.shape, F32),
            pltpu.VMEM(view_data.shape, F32),
            pltpu.VMEM(psf_stack.shape, F32),
            pltpu.VMEM(table.shape, BF),
            pltpu.VMEM((wide, wide, LANES), F32),
            pltpu.VMEM((wide, 2 * lp, LANES), F32),
            pltpu.VMEM((2, nz, 2 * lp, LANES), F32),
            pltpu.VMEM((2, nz, 2 * lp, LANES), F32),
            pltpu.VMEM((nz, 2 * lp, LANES), F32),
            pltpu.VMEM((nz, nx, ny), F32),
            pltpu.VMEM((2, 2, nx, LANES), F32),
            pltpu.VMEM((2, 2, nz, EDGE, ny), F32),
            pltpu.VMEM((2, 2, lx, LANES), F32),
            pltpu.VMEM((1, 8, LANES), F32),
            pltpu.VMEM((8, LANES), F32),
            pltpu.VMEM((LANES, LANES), BF),
            pltpu.VMEM((rows5, LANES), F32),
            pltpu.VMEM((everyone, rows5, LANES), F32),
            pltpu.VMEM((2 * nz * EDGE + 2 * nx + 4 * EDGE, LANES), F32),
            dma((5,)),
            dma((2,)),
            dma((2,)),
            dma((2,)),
            dma((2,)),
            dma,
            dma,
            dma,
            dma,
        ],
        compiler_params=pltpu.CompilerParams(
            collective_id=0, has_side_effects=True, vmem_limit_bytes=48 * 1024 * 1024
        ),
        name="deconvolve",
    )(
        view_index,
        *[
            pltpu.with_memory_space_constraint(a, pltpu.HBM)
            for a in (estimate, view_data, psf_stack, jnp.asarray(table))
        ],
    )
    return pl.pallas_call(
        write_out,
        out_shape=tuple(jax.ShapeDtypeStruct(s, F32) for s in shapes),
        in_specs=[vmem] * 6,
        out_specs=(hbm,) * 6,
        scratch_shapes=[dma((6,))],
        name="write_out",
    )(*[pltpu.with_memory_space_constraint(r, pltpu.VMEM) for r in results])


def solution(mesh):
    return jax.shard_map(
        functools.partial(local, (mesh.shape["gx"], mesh.shape["gy"])),
        mesh=mesh,
        in_specs=(P("gz", "gx", "gy"), P("gz", "gx", "gy"), P(), P()),
        out_specs=(
            P("gz", "gx", "gy"),
            P("gz", "gx", "gy"),
            P("gz", "gx", "gy"),
            P("gz", "gx", "gy"),
            P(None, "gx", "gy"),
            P(),
        ),
        check_vma=False,
    )
```

```python
import functools
import math

import jax
import jax.numpy as jnp
import numpy as np
from jax import lax
from jax.experimental import pallas as pl
from jax.experimental.pallas import tpu as pltpu
from jax.sharding import PartitionSpec as P

MESH = pl.DeviceIdType.MESH
NS = jax.named_scope
BF = jnp.bfloat16
F32 = jnp.float32
LANES = 128
EDGE = 16
GROUP = 8
CORNERS = ((1, 1), (-1, 1), (1, -1), (-1, -1))
SIDES_X = ((1, 0), (-1, 0))
SIDES_Y = ((0, 1), (0, -1))


def two_parts(matrix):
    matrix = np.asarray(matrix, np.float32)
    high = matrix.astype(BF)
    low = (matrix - high.astype(np.float32)).astype(BF)
    return high, low


def split(x):
    high = x.astype(BF)
    return high, (x - high.astype(F32)).astype(BF)


def dot(a, b):
    return jnp.dot(a, b, preferred_element_type=F32)


def tables(nx, ny, extent):
    radius = (extent - 1) // 2
    lx, ly = nx + 2 * EDGE, ny + 2 * EDGE
    nf = ly // 2 + 1
    wide = extent + 1
    freq_y = np.arange(nf)
    freq_x = np.arange(lx)

    def wave(k, n, length):
        return 2 * math.pi / length * np.mod(np.outer(k, n), length)

    pos = np.concatenate([EDGE + np.arange(ny), np.arange(EDGE), EDGE + ny + np.arange(EDGE)])
    fy = np.zeros((ny + 2 * EDGE, 2 * LANES))
    angle = wave(pos, freq_y, ly)
    fy[:, :nf] = np.cos(angle)
    fy[:, LANES : LANES + nf] = -np.sin(angle)
    ky = np.zeros((wide, 2 * LANES))
    angle = wave(np.arange(extent) - radius, freq_y, ly)
    ky[:extent, :nf] = np.cos(angle)
    ky[:extent, LANES : LANES + nf] = -np.sin(angle)
    iy = np.zeros((2 * LANES, ny))
    weight = np.full((nf, 1), 2.0)
    weight[0] = weight[-1] = 1.0
    angle = wave(freq_y, EDGE + np.arange(ny), ly)
    iy[:nf] = weight / ly * np.cos(angle)
    iy[LANES : LANES + nf] = -weight / ly * np.sin(angle)

    angle = wave(freq_x, np.arange(lx), lx)
    fx = np.block([[np.cos(angle), np.sin(angle)], [-np.sin(angle), np.cos(angle)]])
    angle = wave(EDGE + np.arange(nx), freq_x, lx)
    ix = np.block([[np.cos(angle), -np.sin(angle)], [np.sin(angle), np.cos(angle)]]) / lx
    kx = np.zeros((2 * lx, 2, wide))
    angle = wave(freq_x, np.arange(extent) - radius, lx)
    kx[:lx, 0, :extent] = np.cos(angle)
    kx[:lx, 1, :extent] = np.sin(angle)
    kx[lx:, 0, :extent] = -np.sin(angle)
    kx[lx:, 1, :extent] = np.cos(angle)
    kx = kx.reshape(2 * lx, 2 * wide)

    fy_hi, fy_lo = two_parts(fy)
    ky_hi, ky_lo = two_parts(ky)
    iy_hi, iy_lo = two_parts(iy)
    fx_hi, fx_lo = two_parts(fx)
    ix_hi, ix_lo = two_parts(ix)
    kx_hi, kx_lo = two_parts(kx)

    py = np.zeros((ny, LANES))
    px = np.zeros((nx, nx))
    row, col = 0, 0
    places = []
    for level in range(1, 5):
        size = 2**level
        rows, cols = nx // size, ny // size
        places.append((row, rows, col, cols))
        for r in range(rows):
            px[row + r, r * size : (r + 1) * size] = 1.0 / size
        for c in range(cols):
            py[c * size : (c + 1) * size, col + c] = 1.0 / size
        row, col = row + rows, col + cols

    inner = np.concatenate([EDGE + np.arange(nx), lx + EDGE + np.arange(nx)])
    outer = np.setdiff1d(np.arange(2 * lx), inner)
    blank = np.zeros((LANES - 3 * wide, 2 * LANES), BF)
    side_hi, side_lo = fy_hi[ny:], fy_lo[ny:]
    named = {
        "fya": np.concatenate([fy_hi[:ny], fy_hi[:ny]], 0),
        "fyb": np.concatenate([fy_lo[:ny], side_hi, side_hi, side_lo, blank], 0),
        "fxa": np.concatenate([fx_hi[:, inner], fx_hi[:, inner]], 1),
        "fxb": fx_lo[:, inner],
        "fxh": np.concatenate([fx_hi[:, outer], fx_hi[:, outer], fx_lo[:, outer]], 1),
        "ky3": np.concatenate([ky_hi, ky_hi, ky_lo, blank], 0),
        "kx3": np.concatenate([kx_hi, kx_hi, kx_lo], 1),
        "ix2": np.concatenate([ix_hi, ix_lo], 0),
        "iy2": np.concatenate([iy_hi, iy_lo], 1),
        "iy1": iy_hi,
        "py": py.astype(BF),
        "px": px.astype(BF),
    }
    stacked, where, row = [], {}, 0
    for name, a in named.items():
        rows, cols = a.shape
        where[name] = (row, rows, cols)
        full = np.zeros((rows, 2 * LANES), BF)
        full[:, :cols] = a
        stacked.append(full)
        row += rows
    return np.concatenate(stacked, 0), where, tuple(places)


def kernel(
    sizes, where, places,
    index_hbm, est_hbm, view_hbm, psf_hbm, table_hbm,
    out_ref, one_ref, two_ref, three_ref, four_ref, five_ref,
    index_ref, est_ref, view_ref, psf, table,
    psf_pad, k2, own, peer, mix, ratio,
    pack, xhalo, yhalo, share, share_in, place5, mine, tiles, ruler,
    in_sem, hs, hx, hy, es, er, ps, pr, gs, gr,
):
    gxn, gyn = sizes
    nz, nx, ny = est_ref.shape
    extent = psf.shape[1]
    wide = extent + 1
    pairs = nz // 2
    lx = nx + 2 * EDGE
    nf = (ny + 2 * EDGE) // 2 + 1
    third = lx // 3
    lp = 2 * third
    half = (nf + 1) // 2
    middle = (extent - 1) // 2
    gx, gy, gz = lax.axis_index("gx"), lax.axis_index("gy"), lax.axis_index("gz")
    partner = {"gx": gx, "gy": gy, "gz": 1 - gz}
    chips = gxn * gyn
    everyone = 2 * chips

    def tab(name, first=0, count=None):
        row, rows, cols = where[name]
        return table[pl.ds(row + first, rows if count is None else count), pl.ds(0, cols)]

    load_est, load_index, load_psf, load_table, load_view = [
        pltpu.make_async_copy(a, b, in_sem.at[i])
        for i, (a, b) in enumerate(
            (
                (est_hbm, est_ref),
                (index_hbm, index_ref),
                (psf_hbm, psf),
                (table_hbm, table),
                (view_hbm, view_ref),
            )
        )
    ]
    load_est.start()

    def for_others(act):
        zs = (gz, 1 - gz)

        def column(x, ys, skip):
            for b, y in ys:
                for c in range(2):
                    if not (skip and b == 0 and c == 0):
                        act({"gx": x, "gy": y, "gz": zs[c]})

        order = sorted(range(gyn), key=lambda b: -min(b, gyn - b))
        ys = [(b, lax.rem(gy + b, gyn)) for b in order]
        if gxn <= 4:
            for a in (*range(1, gxn), 0):
                column(lax.rem(gx + a, gxn), ys, a == 0)
        else:

            @pl.loop(1, gxn)
            def _(a):
                column(lax.rem(gx + a, gxn), ys, False)

            column(gx, ys, True)

    def signal(device):
        pl.semaphore_signal(barrier, inc=1, device_id=device, device_id_type=MESH)

    barrier = pltpu.get_barrier_semaphore()
    for_others(signal)
    load_psf.start()
    load_index.start()
    load_table.start()
    load_view.start()

    def exists(dx, dy):
        ok = None
        for c, n, d in ((gx, gxn, dx), (gy, gyn, dy)):
            if d > 0:
                t = c < n - 1
            elif d < 0:
                t = c > 0
            else:
                continue
            ok = t if ok is None else jnp.logical_and(ok, t)
        return ok

    def halo_copy(phase, field, dx, dy, planes=None):
        if dy == 0:
            rows = slice(nx - EDGE, nx) if dx > 0 else slice(0, EDGE)
            source = field.at[planes, rows, :]
            target = xhalo.at[phase, 0 if dx > 0 else 1, planes]
        else:
            side = 0 if dy > 0 else 1
            if dx == 0:
                source, target = pack.at[phase, side], yhalo.at[phase, side, pl.ds(EDGE, nx), :]
            else:
                rows = pl.ds(nx - EDGE, EDGE) if dx > 0 else pl.ds(0, EDGE)
                to = pl.ds(0, EDGE) if dx > 0 else pl.ds(EDGE + nx, EDGE)
                source, target = pack.at[phase, side, rows, :], yhalo.at[phase, side, to, :]
        return pltpu.make_async_remote_copy(
            src_ref=source,
            dst_ref=target,
            send_sem=hs.at[phase],
            recv_sem=(hx if dx else hy).at[phase],
            device_id={"gx": gx + dx, "gy": gy + dy, "gz": gz},
            device_id_type=MESH,
        )

    def send_halo(phase, field, directions, planes=None):
        def send(dx, dy, condition=True):
            @pl.when(jnp.logical_and(exists(dx, dy), condition))
            def _():
                halo_copy(phase, field, dx, dy, planes).start()

        odd = lax.rem(gx, 2) == 1
        for dx, dy in directions:
            if dx:
                send(dx, dy, odd if dx > 0 else jnp.logical_not(odd))
        for dx, dy in directions:
            if dx:
                send(dx, dy, odd if dx < 0 else jnp.logical_not(odd))
            else:
                send(dx, dy)

    beside_x = (gx > 0).astype(jnp.int32) + (gx < gxn - 1).astype(jnp.int32)
    beside_y = (gy > 0).astype(jnp.int32) + (gy < gyn - 1).astype(jnp.int32)

    def settle(sem, along_x=True, along_y=True):
        for a in range(3):
            for b in range(3):
                rows = (nz * EDGE * a + EDGE * a * b) * along_x + nx * b * along_y
                if rows:

                    @pl.when(jnp.logical_and(beside_x == a, beside_y == b))
                    def _():
                        part = ruler.at[pl.ds(0, rows)]
                        pltpu.make_async_copy(part, part, sem).wait()

    def add_to_pack(phase, field, planes):
        lane = lax.broadcasted_iota(jnp.int32, (nx, LANES), 1) // EDGE
        for side in range(2):
            kept = pack[phase, side] if planes[0] else jnp.zeros((nx, LANES), F32)
            for z in planes:
                shift = (EDGE * z + EDGE * (1 - side)) % LANES
                moved = pltpu.roll(field[z], shift, 1) if shift else field[z]
                kept = jnp.where(lane == z, moved, kept)
            pack[phase, side] = kept

    def zero_missing(phase):
        for dx, dy in SIDES_X + SIDES_Y + CORNERS:
            if dy == 0:
                target = xhalo.at[phase, 0 if dx > 0 else 1]
            else:
                side = 0 if dy > 0 else 1
                first, count = {0: (EDGE, nx), 1: (0, EDGE), -1: (EDGE + nx, EDGE)}[dx]
                target = yhalo.at[phase, side, pl.ds(first, count), :]

            @pl.when(jnp.logical_not(exists(-dx, -dy)))
            def _():
                target[...] = jnp.zeros(target.shape, F32)

    def swap_copy(phase, first, count):
        planes = pl.ds(first, count)
        return pltpu.make_async_remote_copy(
            src_ref=own.at[phase, planes],
            dst_ref=peer.at[phase, planes],
            send_sem=es.at[phase],
            recv_sem=er.at[phase],
            device_id=partner,
            device_id_type=MESH,
        )

    def fold(x):
        lane = lax.broadcasted_iota(jnp.int32, (lp, LANES), 1)
        rest = x[lp:lx]
        beside = jnp.concatenate(
            [pltpu.roll(rest, nf, 1), pltpu.roll(rest, nf - half, 1)], axis=0
        )
        return jnp.where(lane < nf, x[:lp], beside)

    def unfold(x):
        lane = lax.broadcasted_iota(jnp.int32, (third, LANES), 1)
        low = pltpu.roll(x[:third], LANES - nf, 1)
        high = pltpu.roll(x[third:lp], LANES - (nf - half), 1)
        return jnp.concatenate([x[:lp], jnp.where(lane < half, low, high)], axis=0)

    def beside(phase, z, first, count):
        lane = lax.broadcasted_iota(jnp.int32, (count, LANES), 1)
        left, right = (yhalo[phase, side, pl.ds(first, count), :] for side in range(2))
        if z:
            left = pltpu.roll(left, LANES - EDGE * z, 1)
        if z != 1:
            right = pltpu.roll(right, (EDGE - EDGE * z) % LANES, 1)
        side = jnp.where(lane < EDGE, left, jnp.where(lane < 2 * EDGE, right, 0.0))
        high = side.astype(BF).astype(F32)
        low = side - high
        return (high + pltpu.roll(low, 2 * EDGE, 1) + pltpu.roll(high, 4 * EDGE, 1)).astype(BF)

    def along_y(rows, sides):
        count = len(rows)
        hi, lo = split(jnp.concatenate([jnp.concatenate(r, axis=0) for r in rows], axis=0))
        side = jnp.concatenate([jnp.concatenate(r, axis=0) for r in sides], axis=0)
        x1 = dot(jnp.concatenate([hi, lo], axis=1), tab("fya")) + dot(
            jnp.concatenate([hi, side], axis=1), tab("fyb")
        )
        n = x1.shape[0] // count
        stacked = [
            jnp.concatenate([x1[k * n : (k + 1) * n, :LANES], x1[k * n : (k + 1) * n, LANES:]], 0)
            for k in range(count)
        ]
        return [split(jnp.concatenate(stacked[k : k + 2], axis=1)) for k in range(0, count, 2)]

    def forward(phase, field, planes):
        spectra = along_y(
            [[field[z]] for z in planes], [[beside(phase, z, EDGE, nx)] for z in planes]
        )
        for q, (hi, lo) in enumerate(spectra):
            x2 = dot(tab("fxa"), jnp.concatenate([hi, lo], axis=0)) + dot(tab("fxb"), hi)
            for k in range(2):
                z = planes[2 * q + k]
                part = x2[:, k * LANES : (k + 1) * LANES]
                mix[z] = part

    def forward_edges(phase, planes):
        spectra = along_y(
            [[xhalo[phase, side, z] for side in range(2)] for z in planes],
            [[beside(phase, z, first, EDGE) for first in (0, EDGE + nx)] for z in planes],
        )
        for q, (hi, lo) in enumerate(spectra):
            x2 = dot(tab("fxh"), jnp.concatenate([hi, lo, hi], axis=0))
            for k in range(2):
                z = planes[2 * q + k]
                part = mix[z] + x2[:, k * LANES : (k + 1) * LANES]
                own[phase, z, pl.ds(0, lp), :] = fold(part[:lx])
                own[phase, z, pl.ds(lp, lp), :] = fold(part[lx:])

    def mix_planes(source, phase, base, conj, add, chosen):
        @pl.loop(0, lp // 8)
        def _(s):
            re = pl.ds(pl.multiple_of(s * 8, 8), 8)
            im = pl.ds(pl.multiple_of(lp + s * 8, 8), 8)
            vr = [source[phase, j, re, :] for j in range(nz)]
            vi = [source[phase, j, im, :] for j in range(nz)]
            kr, ki = {}, {}
            reach = [(j - i if conj else i - j) for i in chosen for j in range(nz)]
            for d in sorted(set(reach)):
                kr[d] = k2[base + d, re, :]
                ki[d] = k2[base + d, im, :]
            ks = {d: kr[d] - ki[d] if conj else kr[d] + ki[d] for d in kr}
            vs = [r + i for r, i in zip(vr, vi)]
            for i in chosen:
                a = b = c = None
                for j in range(nz):
                    d = j - i if conj else i - j
                    rr, ii, ss = kr[d] * vr[j], ki[d] * vi[j], ks[d] * vs[j]
                    a = rr if a is None else a + rr
                    b = ii if b is None else b + ii
                    c = ss if c is None else c + ss
                yr = a + b if conj else a - b
                yi = c - a + b if conj else c - a - b
                mix[i, re, :] = mix[i, re, :] + yr if add else yr
                mix[i, im, :] = mix[i, im, :] + yi if add else yi

    def inverse(planes, write):
        rows = []
        for z in planes[::2]:
            y = jnp.concatenate(
                [
                    jnp.concatenate([unfold(mix[w, pl.ds(0, lp)]), unfold(mix[w, pl.ds(lp, lp)])], 0)
                    for w in (z, z + 1)
                ],
                axis=1,
            )
            hi, lo = split(y)
            both = dot(tab("ix2"), hi)
            g = both[: 2 * nx] + both[2 * nx :] + dot(tab("ix2", 0, 2 * nx), lo)
            for k in range(2):
                part = g[:, k * LANES : (k + 1) * LANES]
                rows.append(jnp.concatenate([part[:nx], part[nx:]], axis=1))
        hi, lo = split(jnp.concatenate(rows, axis=0))
        both = dot(hi, tab("iy2"))
        field = both[:, :ny] + both[:, ny:] + dot(lo, tab("iy1"))
        for k, z in enumerate(planes):
            write(z, field[k * nx : (k + 1) * nx])

    def prepare(first):
        block = psf_pad[pl.ds(first, GROUP)].reshape(GROUP * wide, LANES)
        high = block.astype(BF).astype(F32)
        low = block - high
        x1 = dot(
            (high + pltpu.roll(low, wide, 1) + pltpu.roll(high, 2 * wide, 1)).astype(BF),
            tab("ky3"),
        )
        hi, lo = split(x1)
        hi = hi.reshape(GROUP, wide, 2 * LANES)
        lo = lo.reshape(GROUP, wide, 2 * LANES)
        for h in range(GROUP // 2):
            columns = []
            for n in (2 * h, 2 * h + 1):
                parts = []
                for part in (hi[n], lo[n], hi[n]):
                    parts.append(part[:, :LANES])
                    parts.append(part[:, LANES:])
                columns.append(jnp.concatenate(parts, axis=0))
            spectrum = dot(tab("kx3"), jnp.concatenate(columns, axis=1))
            for n in range(2):
                part = spectrum[:, n * LANES : (n + 1) * LANES]
                k2[first + 2 * h + n, pl.ds(0, lp), :] = fold(part[:lx])
                k2[first + 2 * h + n, pl.ds(lp, lp), :] = fold(part[lx:])

    def convolve(phase, field, conj, groups, write, after):
        with NS(f"wait_haloy{phase}"):
            settle(hy.at[phase], along_x=False)
        with NS(f"forward{phase}"):
            for z in range(0, nz, 8):
                forward(phase, field, range(z, z + 8))
        with NS(f"wait_halox{phase}"):
            settle(hx.at[phase], along_y=False)
        with NS(f"edges{phase}"):
            for first, count in ((0, 8),):
                forward_edges(phase, range(first, first + count))
                swap_copy(phase, first, count).start()
        sign = 1 - 2 * gz if conj else 2 * gz - 1
        with NS(f"mixown{phase}"):
            mix_planes(own, phase, middle, conj, False, range(nz))
        if phase == 0:
            with NS("prepare2"):
                prepare(3 * GROUP * gz)
        with NS(f"waitswap{phase}"):
            pltpu.make_async_copy(own.at[phase], peer.at[phase], er.at[phase]).wait()
        with NS(f"mixpeer{phase}"):
            mix_planes(peer, phase, middle + sign * nz, conj, True, range(nz))
        size = nz // groups
        for n in range(groups):
            planes = range(n * size, (n + 1) * size)
            with NS(f"inverse{phase}_{n}"):
                inverse(planes, write)
                after(planes)

    with NS("zero"):
        zero_missing(0)
        zero_missing(1)
    with NS("wait_est"):
        load_est.wait()
    with NS("pack0"):
        add_to_pack(0, est_ref, range(nz))
    with NS("barrier"):
        pl.semaphore_wait(barrier, everyone - 1)
    with NS("send0"):
        send_halo(0, est_ref, SIDES_Y)
        send_halo(0, est_ref, CORNERS)
        send_halo(0, est_ref, SIDES_X, pl.ds(0, nz))

    with NS("wait_loads"):
        load_index.wait()
        load_psf.wait()
        load_table.wait()
        load_view.wait()
    with NS("psf_prep"):
        chosen = psf[index_ref[0]]
        total = jnp.sum(chosen, axis=0)
        total = jnp.sum(jnp.sum(total, axis=1, keepdims=True), axis=0, keepdims=True)
        psf_pad[...] = jnp.zeros(psf_pad.shape, F32)
        psf_pad[pl.ds(0, extent), pl.ds(0, extent), pl.ds(0, extent)] = (
            chosen * (1.0 / total)[None]
        )

    with NS("prepare1"):

        @pl.loop(1, 3)
        def _(g):
            prepare(g * GROUP)

    def write_ratio(z, blurred):
        ratio[z] = view_ref[z] / blurred

    def after_ratio(planes):
        add_to_pack(1, ratio, planes)
        if planes[-1] == nz - 1:
            send_halo(1, ratio, SIDES_Y)
        if planes[-1] == nz - 1:
            send_halo(1, ratio, CORNERS)
        send_halo(1, ratio, SIDES_X, pl.ds(planes[0], len(planes)))

    convolve(0, est_ref, False, 2, write_ratio, after_ratio)

    with NS("prepare3"):
        prepare(3 * GROUP * (1 - gz))
        cols5 = four_ref.shape[2] // 2
        i = lax.broadcasted_iota(jnp.int32, (LANES, LANES), 0)
        j = lax.broadcasted_iota(jnp.int32, (LANES, LANES), 1)
        target = i // (ny // cols5) + gy * cols5
        place5[...] = jnp.where(j == target, 1.0 / (nz * 2 * 32 * 32), 0.0).astype(BF)

    def write_update(z, correction):
        out_ref[z] = est_ref[z] * correction

    convolve(1, ratio, True, 1, write_update, lambda planes: None)

    with NS("five_send"):
        rows5 = four_ref.shape[1] // 2
        total = out_ref[0]
        for z in range(1, nz):
            total = total + out_ref[z]
        summed = jnp.sum(total.reshape(rows5, nx // rows5, ny), axis=1)
        hi, lo = split(summed)
        mine[...] = dot(hi, place5[...]) + dot(lo, place5[...])

        def slot(x, y, z):
            return (x * gyn + y) * 2 + z

        def send_tile(device):
            pltpu.make_async_remote_copy(
                src_ref=mine,
                dst_ref=tiles.at[slot(gx, gy, gz)],
                send_sem=gs,
                recv_sem=gr,
                device_id=device,
                device_id_type=MESH,
            ).start()

        for_others(send_tile)
        tiles[slot(gx, gy, gz)] = mine[...]

    def pooled(plane):
        hi, lo = split(plane)
        t = dot(hi, tab("py")) + dot(lo, tab("py"))
        hi, lo = split(t)
        return dot(tab("px"), hi) + dot(tab("px"), lo)

    with NS("pyramid"):
        halves = [(out_ref[2 * i] + out_ref[2 * i + 1]) * 0.5 for i in range(nz // 2)]
        quarters = [(halves[2 * i] + halves[2 * i + 1]) * 0.5 for i in range(nz // 4)]
        eighth = (quarters[0] + quarters[1]) * 0.5
        r4, c4 = places[3][0], places[3][2]
        last = pooled(eighth)
        share[0] = last[r4 : r4 + 8]
        share_copy = pltpu.make_async_remote_copy(
            src_ref=share.at[0], dst_ref=share_in, send_sem=ps, recv_sem=pr,
            device_id=partner, device_id_type=MESH,
        )
        share_copy.start()
        row, rows, col, cols = places[2]
        three_ref[0] = last[row : row + rows, col : col + cols]
        row, rows, col, cols = places[1]
        for i, plane in enumerate(quarters):
            two_ref[i] = pooled(plane)[row : row + rows, col : col + cols]
        row, rows, col, cols = places[0]
        for i, plane in enumerate(halves):
            one_ref[i] = pooled(plane)[row : row + rows, col : col + cols]
    with NS("share"):
        share_copy.wait()
        both = (share[0] + share_in[...]) * 0.5
        four_ref[0] = both[: places[3][1], c4 : c4 + places[3][3]]
    with NS("settle"):
        for phase in range(2):
            settle(hs.at[phase])
            pltpu.make_async_copy(own.at[phase], peer.at[phase], es.at[phase]).wait()
    with NS("wait_tiles"):
        others = tiles.at[pl.ds(0, everyone - 1)]
        pltpu.make_async_copy(others, others, gs).wait()
        pltpu.make_async_copy(others, others, gr).wait()
    with NS("five"):
        for x in range(gxn):
            five = tiles[slot(x, 0, 0)]
            for n in range(1, 2 * gyn):
                five = five + tiles[slot(x, 0, 0) + n]
            five_ref[0, pl.ds(x * rows5, rows5), :] = five[:, : five_ref.shape[2]]


def write_out(*refs):
    sems = refs[12]
    copies = [pltpu.make_async_copy(refs[i], refs[6 + i], sems.at[i]) for i in range(6)]
    for copy in copies:
        copy.start()
    for copy in copies:
        copy.wait()


def local(sizes, estimate, view_data, psf_stack, view_index):
    gxn, gyn = sizes
    nz, nx, ny = estimate.shape
    extent = psf_stack.shape[1]
    table, where, places = tables(nx, ny, extent)
    lx = nx + 2 * EDGE
    lp = 2 * (lx // 3)
    wide = extent + 1
    everyone = 2 * gxn * gyn
    vmem = pl.BlockSpec(memory_space=pltpu.VMEM)
    hbm = pl.BlockSpec(memory_space=pltpu.HBM)
    rows5, cols5 = nx // 32, ny // 32
    dma = pltpu.SemaphoreType.DMA
    shapes = (
        (nz, nx, ny),
        (nz // 2, nx // 2, ny // 2),
        (nz // 4, nx // 4, ny // 4),
        (nz // 8, nx // 8, ny // 8),
        (1, nx // 16, ny // 16),
        (1, rows5 * gxn, cols5 * gyn),
    )
    results = pl.pallas_call(
        functools.partial(kernel, sizes, where, places),
        out_shape=tuple(pltpu.VMEM(s, F32) for s in shapes),
        in_specs=[hbm] * 5,
        out_specs=(vmem,) * 6,
        scratch_shapes=[
            pltpu.SMEM(view_index.shape, view_index.dtype),
            pltpu.VMEM(estimate.shape, F32),
            pltpu.VMEM(view_data.shape, F32),
            pltpu.VMEM(psf_stack.shape, F32),
            pltpu.VMEM(table.shape, BF),
            pltpu.VMEM((wide, wide, LANES), F32),
            pltpu.VMEM((wide, 2 * lp, LANES), F32),
            pltpu.VMEM((2, nz, 2 * lp, LANES), F32),
            pltpu.VMEM((2, nz, 2 * lp, LANES), F32),
            pltpu.VMEM((nz, 2 * lx, LANES), F32),
            pltpu.VMEM((nz, nx, ny), F32),
            pltpu.VMEM((2, 2, nx, LANES), F32),
            pltpu.VMEM((2, 2, nz, EDGE, ny), F32),
            pltpu.VMEM((2, 2, lx, LANES), F32),
            pltpu.VMEM((1, 8, LANES), F32),
            pltpu.VMEM((8, LANES), F32),
            pltpu.VMEM((LANES, LANES), BF),
            pltpu.VMEM((rows5, LANES), F32),
            pltpu.VMEM((everyone, rows5, LANES), F32),
            pltpu.VMEM((2 * nz * EDGE + 2 * nx + 4 * EDGE, LANES), F32),
            dma((5,)),
            dma((2,)),
            dma((2,)),
            dma((2,)),
            dma((2,)),
            dma((2,)),
            dma,
            dma,
            dma,
            dma,
        ],
        compiler_params=pltpu.CompilerParams(
            collective_id=0, has_side_effects=True, vmem_limit_bytes=48 * 1024 * 1024
        ),
        name="deconvolve",
    )(
        view_index,
        *[
            pltpu.with_memory_space_constraint(a, pltpu.HBM)
            for a in (estimate, view_data, psf_stack, jnp.asarray(table))
        ],
    )
    return pl.pallas_call(
        write_out,
        out_shape=tuple(jax.ShapeDtypeStruct(s, F32) for s in shapes),
        in_specs=[vmem] * 6,
        out_specs=(hbm,) * 6,
        scratch_shapes=[dma((6,))],
        name="write_out",
    )(*[pltpu.with_memory_space_constraint(r, pltpu.VMEM) for r in results])


def solution(mesh):
    return jax.shard_map(
        functools.partial(local, (mesh.shape["gx"], mesh.shape["gy"])),
        mesh=mesh,
        in_specs=(P("gz", "gx", "gy"), P("gz", "gx", "gy"), P(), P()),
        out_specs=(
            P("gz", "gx", "gy"),
            P("gz", "gx", "gy"),
            P("gz", "gx", "gy"),
            P("gz", "gx", "gy"),
            P(None, "gx", "gy"),
            P(),
        ),
        check_vma=False,
    )
```

```python
import functools
import math

import jax
import jax.numpy as jnp
import numpy as np
from jax import lax
from jax.experimental import pallas as pl
from jax.experimental.pallas import tpu as pltpu
from jax.sharding import PartitionSpec as P

MESH = pl.DeviceIdType.MESH
NS = jax.named_scope
BF = jnp.bfloat16
F32 = jnp.float32
LANES = 128
EDGE = 16
GROUP = 8
CHUNKS = 4
STEPS = ((0, 8),)
CORNERS = ((1, 1), (-1, 1), (1, -1), (-1, -1))
SIDES_X = ((1, 0), (-1, 0))
SIDES_Y = ((0, 1), (0, -1))


def two_parts(matrix):
    matrix = np.asarray(matrix, np.float32)
    high = matrix.astype(BF)
    low = (matrix - high.astype(np.float32)).astype(BF)
    return high, low


def split(x):
    high = x.astype(BF)
    return high, (x - high.astype(F32)).astype(BF)


def dot(a, b):
    return jnp.dot(a, b, preferred_element_type=F32)


def tables(nx, ny, extent):
    radius = (extent - 1) // 2
    lx, ly = nx + 2 * EDGE, ny + 2 * EDGE
    nf = ly // 2 + 1
    wide = extent + 1
    freq_y = np.arange(nf)
    freq_x = np.arange(lx)

    def wave(k, n, length):
        return 2 * math.pi / length * np.mod(np.outer(k, n), length)

    pos = np.concatenate([EDGE + np.arange(ny), np.arange(EDGE), EDGE + ny + np.arange(EDGE)])
    fy = np.zeros((ny + 2 * EDGE, 2 * LANES))
    angle = wave(pos, freq_y, ly)
    fy[:, :nf] = np.cos(angle)
    fy[:, LANES : LANES + nf] = -np.sin(angle)
    ky = np.zeros((wide, 2 * LANES))
    angle = wave(np.arange(extent) - radius, freq_y, ly)
    ky[:extent, :nf] = np.cos(angle)
    ky[:extent, LANES : LANES + nf] = -np.sin(angle)
    iy = np.zeros((2 * LANES, ny))
    weight = np.full((nf, 1), 2.0)
    weight[0] = weight[-1] = 1.0
    angle = wave(freq_y, EDGE + np.arange(ny), ly)
    iy[:nf] = weight / ly * np.cos(angle)
    iy[LANES : LANES + nf] = -weight / ly * np.sin(angle)

    angle = wave(freq_x, np.arange(lx), lx)
    fx = np.block([[np.cos(angle), np.sin(angle)], [-np.sin(angle), np.cos(angle)]])
    angle = wave(EDGE + np.arange(nx), freq_x, lx)
    ix = np.block([[np.cos(angle), -np.sin(angle)], [np.sin(angle), np.cos(angle)]]) / lx
    kx = np.zeros((2 * lx, 2, wide))
    angle = wave(freq_x, np.arange(extent) - radius, lx)
    kx[:lx, 0, :extent] = np.cos(angle)
    kx[:lx, 1, :extent] = np.sin(angle)
    kx[lx:, 0, :extent] = -np.sin(angle)
    kx[lx:, 1, :extent] = np.cos(angle)
    kx = kx.reshape(2 * lx, 2 * wide)

    fy_hi, fy_lo = two_parts(fy)
    ky_hi, ky_lo = two_parts(ky)
    iy_hi, iy_lo = two_parts(iy)
    fx_hi, fx_lo = two_parts(fx)
    ix_hi, ix_lo = two_parts(ix)
    kx_hi, kx_lo = two_parts(kx)

    py = np.zeros((ny, LANES))
    px = np.zeros((nx, nx))
    row, col = 0, 0
    places = []
    for level in range(1, 5):
        size = 2**level
        rows, cols = nx // size, ny // size
        places.append((row, rows, col, cols))
        for r in range(rows):
            px[row + r, r * size : (r + 1) * size] = 1.0 / size
        for c in range(cols):
            py[c * size : (c + 1) * size, col + c] = 1.0 / size
        row, col = row + rows, col + cols

    inner = np.concatenate([EDGE + np.arange(nx), lx + EDGE + np.arange(nx)])
    outer = np.setdiff1d(np.arange(2 * lx), inner)
    x_edge = np.concatenate([np.arange(EDGE), nx - EDGE + np.arange(EDGE)])
    x_middle = EDGE + np.arange(nx - 2 * EDGE)
    inverse_rows = np.concatenate([x_edge, nx + x_edge, x_middle, nx + x_middle])
    blank = np.zeros((LANES - 3 * wide, 2 * LANES), BF)
    side_hi, side_lo = fy_hi[ny:], fy_lo[ny:]
    named = {
        "fya": np.concatenate([fy_hi[:ny], fy_hi[:ny]], 0),
        "fyb": np.concatenate([fy_lo[:ny], side_hi, side_hi, side_lo, blank], 0),
        "fxa": np.concatenate([fx_hi[:, inner], fx_hi[:, inner]], 1),
        "fxb": fx_lo[:, inner],
        "fxh": np.concatenate([fx_hi[:, outer], fx_hi[:, outer], fx_lo[:, outer]], 1),
        "ky3": np.concatenate([ky_hi, ky_hi, ky_lo, blank], 0),
        "kx3": np.concatenate([kx_hi, kx_hi, kx_lo], 1),
        "ix2": np.concatenate([part[inverse_rows] for part in (ix_hi, ix_lo)], 0),
        "iy2": np.concatenate([iy_hi, iy_lo], 1),
        "iy1": iy_hi,
        "py": py.astype(BF),
        "px": px.astype(BF),
    }
    stacked, where, row = [], {}, 0
    for name, a in named.items():
        rows, cols = a.shape
        where[name] = (row, rows, cols)
        full = np.zeros((rows, 2 * LANES), BF)
        full[:, :cols] = a
        stacked.append(full)
        row += rows
    return np.concatenate(stacked, 0), where, tuple(places)


def kernel(
    sizes, where, places,
    index_hbm, est_hbm, view_hbm, psf_hbm, table_hbm,
    out_ref, one_ref, two_ref, three_ref, four_ref, five_ref,
    index_ref, est_ref, view_ref, psf, table,
    psf_pad, k2, own, peer, mix, parts_of, ratio,
    pack, xhalo, yhalo, share, share_in, place5, mine, tiles, ruler,
    in_sem, hs, hx, hy, es, er, ps, pr, gs, gr,
):
    gxn, gyn = sizes
    nz, nx, ny = est_ref.shape
    extent = psf.shape[1]
    wide = extent + 1
    pairs = nz // 2
    lx = nx + 2 * EDGE
    nf = (ny + 2 * EDGE) // 2 + 1
    third = lx // 3
    lp = 2 * third
    half = (nf + 1) // 2
    middle = (extent - 1) // 2
    gx, gy, gz = lax.axis_index("gx"), lax.axis_index("gy"), lax.axis_index("gz")
    partner = {"gx": gx, "gy": gy, "gz": 1 - gz}
    chips = gxn * gyn
    everyone = 2 * chips

    def tab(name, first=0, count=None):
        row, rows, cols = where[name]
        return table[pl.ds(row + first, rows if count is None else count), pl.ds(0, cols)]

    load_est, load_index, load_psf, load_table, load_view = [
        pltpu.make_async_copy(a, b, in_sem.at[i])
        for i, (a, b) in enumerate(
            (
                (est_hbm, est_ref),
                (index_hbm, index_ref),
                (psf_hbm, psf),
                (table_hbm, table),
                (view_hbm, view_ref),
            )
        )
    ]
    load_est.start()

    def for_others(act):
        zs = (gz, 1 - gz)

        def column(x, ys, skip):
            for b, y in ys:
                for c in range(2):
                    if not (skip and b == 0 and c == 0):
                        act({"gx": x, "gy": y, "gz": zs[c]})

        order = sorted(range(gyn), key=lambda b: -min(b, gyn - b))
        ys = [(b, lax.rem(gy + b, gyn)) for b in order]
        if gxn <= 4:
            for a in (*range(1, gxn), 0):
                column(lax.rem(gx + a, gxn), ys, a == 0)
        else:

            @pl.loop(1, gxn)
            def _(a):
                column(lax.rem(gx + a, gxn), ys, False)

            column(gx, ys, True)

    def signal(device):
        pl.semaphore_signal(barrier, inc=1, device_id=device, device_id_type=MESH)

    def exists(dx, dy):
        ok = None
        for c, n, d in ((gx, gxn, dx), (gy, gyn, dy)):
            if d > 0:
                t = c < n - 1
            elif d < 0:
                t = c > 0
            else:
                continue
            ok = t if ok is None else jnp.logical_and(ok, t)
        return ok

    beside_x = (gx > 0).astype(jnp.int32) + (gx < gxn - 1).astype(jnp.int32)
    beside_y = (gy > 0).astype(jnp.int32) + (gy < gyn - 1).astype(jnp.int32)

    barrier = pltpu.get_barrier_semaphore()
    close = max(gxn, gyn) <= 4
    if close:
        signal(partner)
        for dx, dy in SIDES_X + SIDES_Y + CORNERS:

            @pl.when(exists(dx, dy))
            def _():
                signal({"gx": gx + dx, "gy": gy + dy, "gz": gz})
    else:
        for_others(signal)
    load_psf.start()
    load_index.start()
    load_table.start()
    load_view.start()

    def halo_copy(phase, field, dx, dy, planes=None):
        if dy == 0:
            rows = slice(nx - EDGE, nx) if dx > 0 else slice(0, EDGE)
            source = field.at[planes, rows, :]
            target = xhalo.at[phase, 0 if dx > 0 else 1, planes]
        else:
            side = 0 if dy > 0 else 1
            if dx == 0:
                source, target = pack.at[phase, side], yhalo.at[phase, side, pl.ds(EDGE, nx), :]
            else:
                rows = pl.ds(nx - EDGE, EDGE) if dx > 0 else pl.ds(0, EDGE)
                to = pl.ds(0, EDGE) if dx > 0 else pl.ds(EDGE + nx, EDGE)
                source, target = pack.at[phase, side, rows, :], yhalo.at[phase, side, to, :]
        return pltpu.make_async_remote_copy(
            src_ref=source,
            dst_ref=target,
            send_sem=hs.at[phase],
            recv_sem=(hx if dx else hy).at[phase],
            device_id={"gx": gx + dx, "gy": gy + dy, "gz": gz},
            device_id_type=MESH,
        )

    def send_halo(phase, field, directions, planes=None):
        def send(dx, dy, condition=True):
            @pl.when(jnp.logical_and(exists(dx, dy), condition))
            def _():
                halo_copy(phase, field, dx, dy, planes).start()

        odd = lax.rem(gx, 2) == 1
        for dx, dy in directions:
            if dx:
                send(dx, dy, odd if dx > 0 else jnp.logical_not(odd))
        for dx, dy in directions:
            if dx:
                send(dx, dy, odd if dx < 0 else jnp.logical_not(odd))
            else:
                send(dx, dy)

    def settle(sem, along_x=True, along_y=True):
        for a in range(3):
            for b in range(3):
                rows = (nz * EDGE * a + EDGE * a * b) * along_x + nx * b * along_y
                if rows:

                    @pl.when(jnp.logical_and(beside_x == a, beside_y == b))
                    def _():
                        part = ruler.at[pl.ds(0, rows)]
                        pltpu.make_async_copy(part, part, sem).wait()

    def do_pack(phase, field, rows):
        count = rows.size
        lane = lax.broadcasted_iota(jnp.int32, (count, LANES), 1) // EDGE
        for side in range(2):
            packed = jnp.zeros((count, LANES), F32)
            for z in range(nz):
                shift = (EDGE * z + EDGE * (1 - side)) % LANES
                cells = field[z, rows, :]
                packed = jnp.where(lane == z, pltpu.roll(cells, shift, 1) if shift else cells, packed)
            pack[phase, side, rows, :] = packed

    def zero_missing(phase):
        for dx, dy in SIDES_X + SIDES_Y + CORNERS:
            if dy == 0:
                target = xhalo.at[phase, 0 if dx > 0 else 1]
            else:
                side = 0 if dy > 0 else 1
                first, count = {0: (EDGE, nx), 1: (0, EDGE), -1: (EDGE + nx, EDGE)}[dx]
                target = yhalo.at[phase, side, pl.ds(first, count), :]

            @pl.when(jnp.logical_not(exists(-dx, -dy)))
            def _():
                target[...] = jnp.zeros(target.shape, F32)

    def swap_copy(phase, n):
        planes = pl.ds(n * nz // CHUNKS, nz // CHUNKS)
        return pltpu.make_async_remote_copy(
            src_ref=own.at[phase, planes],
            dst_ref=peer.at[phase, planes],
            send_sem=es.at[phase],
            recv_sem=er.at[phase, n],
            device_id=partner,
            device_id_type=MESH,
        )

    def fold(x):
        lane = lax.broadcasted_iota(jnp.int32, (lp, LANES), 1)
        rest = x[lp:lx]
        beside = jnp.concatenate(
            [pltpu.roll(rest, nf, 1), pltpu.roll(rest, nf - half, 1)], axis=0
        )
        return jnp.where(lane < nf, x[:lp], beside)

    def unfold(x):
        lane = lax.broadcasted_iota(jnp.int32, (third, LANES), 1)
        low = pltpu.roll(x[:third], LANES - nf, 1)
        high = pltpu.roll(x[third:lp], LANES - (nf - half), 1)
        return jnp.concatenate([x[:lp], jnp.where(lane < half, low, high)], axis=0)

    def beside(phase, z, first, count):
        lane = lax.broadcasted_iota(jnp.int32, (count, LANES), 1)
        left, right = (yhalo[phase, side, pl.ds(first, count), :] for side in range(2))
        if z:
            left = pltpu.roll(left, LANES - EDGE * z, 1)
        if z != 1:
            right = pltpu.roll(right, (EDGE - EDGE * z) % LANES, 1)
        side = jnp.where(lane < EDGE, left, jnp.where(lane < 2 * EDGE, right, 0.0))
        high = side.astype(BF).astype(F32)
        low = side - high
        return (high + pltpu.roll(low, 2 * EDGE, 1) + pltpu.roll(high, 4 * EDGE, 1)).astype(BF)

    def along_y(rows, sides):
        count = len(rows)
        hi, lo = split(jnp.concatenate([jnp.concatenate(r, axis=0) for r in rows], axis=0))
        side = jnp.concatenate([jnp.concatenate(r, axis=0) for r in sides], axis=0)
        x1 = dot(jnp.concatenate([hi, lo], axis=1), tab("fya")) + dot(
            jnp.concatenate([hi, side], axis=1), tab("fyb")
        )
        n = x1.shape[0] // count
        stacked = [
            jnp.concatenate([x1[k * n : (k + 1) * n, :LANES], x1[k * n : (k + 1) * n, LANES:]], 0)
            for k in range(count)
        ]
        return [split(jnp.concatenate(stacked[k : k + 2], axis=1)) for k in range(0, count, 2)]

    def forward(phase, field, planes):
        spectra = along_y(
            [[field[z]] for z in planes], [[beside(phase, z, EDGE, nx)] for z in planes]
        )
        for q, (hi, lo) in enumerate(spectra):
            x2 = dot(tab("fxa"), jnp.concatenate([hi, lo], axis=0)) + dot(tab("fxb"), hi)
            for k in range(2):
                z = planes[2 * q + k]
                part = x2[:, k * LANES : (k + 1) * LANES]
                mix[z] = part

    def forward_edges(phase, planes):
        spectra = along_y(
            [[xhalo[phase, side, z] for side in range(2)] for z in planes],
            [[beside(phase, z, first, EDGE) for first in (0, EDGE + nx)] for z in planes],
        )
        for q, (hi, lo) in enumerate(spectra):
            x2 = dot(tab("fxh"), jnp.concatenate([hi, lo, hi], axis=0))
            for k in range(2):
                z = planes[2 * q + k]
                part = mix[z] + x2[:, k * LANES : (k + 1) * LANES]
                own[phase, z, pl.ds(0, lp), :] = fold(part[:lx])
                own[phase, z, pl.ds(lp, lp), :] = fold(part[lx:])

    def mix_planes(source, phase, base, conj, add, taken):
        @pl.loop(0, lp // 8)
        def _(s):
            re = pl.ds(pl.multiple_of(s * 8, 8), 8)
            im = pl.ds(pl.multiple_of(lp + s * 8, 8), 8)
            vr = {j: source[phase, j, re, :] for j in taken}
            vi = {j: source[phase, j, im, :] for j in taken}
            kr, ki = {}, {}
            for d in sorted({j - i if conj else i - j for i in range(nz) for j in taken}):
                kr[d] = k2[base + d, re, :]
                ki[d] = k2[base + d, im, :]
            ks = {d: kr[d] - ki[d] if conj else kr[d] + ki[d] for d in kr}
            vs = {j: vr[j] + vi[j] for j in taken}
            for i in range(nz):
                a = b = c = None
                for j in taken:
                    d = j - i if conj else i - j
                    rr, ii, ss = kr[d] * vr[j], ki[d] * vi[j], ks[d] * vs[j]
                    a = rr if a is None else a + rr
                    b = ii if b is None else b + ii
                    c = ss if c is None else c + ss
                yr = a + b if conj else a - b
                yi = c - a + b if conj else c - a - b
                mix[i, re, :] = mix[i, re, :] + yr if add else yr
                mix[i, im, :] = mix[i, im, :] + yi if add else yi

    segments = (((0, EDGE), (nx - EDGE, EDGE)), ((EDGE, nx - 2 * EDGE),))

    def unfolded(z):
        return jnp.concatenate([unfold(mix[z, pl.ds(0, lp)]), unfold(mix[z, pl.ds(lp, lp)])], 0)

    def inverse(planes, parts, write, keep=False, kept=False):
        counts = [sum(count for _, count in segments[p]) for p in parts]
        offset = 2 * sum(count for _, count in segments[0]) * parts[0]
        rows = []
        for z in planes[::2]:
            if kept:
                hi, lo = parts_of[z // 2, 0], parts_of[z // 2, 1]
            else:
                hi, lo = split(jnp.concatenate([unfolded(z), unfolded(z + 1)], axis=1))
            if keep:
                parts_of[z // 2, 0] = hi
                parts_of[z // 2, 1] = lo
            high = tab("ix2", offset, 2 * sum(counts))
            g = dot(high, hi) + dot(tab("ix2", 2 * nx + offset, 2 * sum(counts)), hi) + dot(high, lo)
            for k in range(2):
                part = g[:, k * LANES : (k + 1) * LANES]
                for count in counts:
                    rows.append(jnp.concatenate([part[:count], part[count : 2 * count]], axis=1))
                    part = part[2 * count :]
        hi, lo = split(jnp.concatenate(rows, axis=0))
        both = dot(hi, tab("iy2"))
        values = both[:, :ny] + both[:, ny:] + dot(lo, tab("iy1"))
        row = 0
        for z in planes:
            for p in parts:
                for first, count in segments[p]:
                    write(z, pl.ds(first, count), values[row : row + count])
                    row += count

    def prepare(first):
        block = psf_pad[pl.ds(first, GROUP)].reshape(GROUP * wide, LANES)
        high = block.astype(BF).astype(F32)
        low = block - high
        x1 = dot(
            (high + pltpu.roll(low, wide, 1) + pltpu.roll(high, 2 * wide, 1)).astype(BF),
            tab("ky3"),
        )
        hi, lo = split(x1)
        hi = hi.reshape(GROUP, wide, 2 * LANES)
        lo = lo.reshape(GROUP, wide, 2 * LANES)
        for h in range(GROUP // 2):
            columns = []
            for n in (2 * h, 2 * h + 1):
                parts = []
                for part in (hi[n], lo[n], hi[n]):
                    parts.append(part[:, :LANES])
                    parts.append(part[:, LANES:])
                columns.append(jnp.concatenate(parts, axis=0))
            spectrum = dot(tab("kx3"), jnp.concatenate(columns, axis=1))
            for n in range(2):
                part = spectrum[:, n * LANES : (n + 1) * LANES]
                k2[first + 2 * h + n, pl.ds(0, lp), :] = fold(part[:lx])
                k2[first + 2 * h + n, pl.ds(lp, lp), :] = fold(part[lx:])

    def convolve(phase, field, conj, invert):
        with NS(f"wait_haloy{phase}"):
            settle(hy.at[phase], along_x=False)
        with NS(f"forward{phase}"):
            for z in range(0, nz, 8):
                forward(phase, field, range(z, z + 8))
        if phase == 0:
            with NS("prepare2"):
                prepare(3 * GROUP * gz)
        with NS(f"wait_halox{phase}"):
            settle(hx.at[phase], along_y=False)
        with NS(f"edges{phase}"):
            forward_edges(phase, range(nz))
            for n in range(CHUNKS):
                swap_copy(phase, n).start()
        sign = 1 - 2 * gz if conj else 2 * gz - 1
        with NS(f"mixown{phase}"):
            mix_planes(own, phase, middle, conj, False, range(nz))
        for n in range(CHUNKS):
            with NS(f"waitswap{phase}_{n}"):
                swap_copy(phase, n).wait_recv()
            with NS(f"mixpeer{phase}_{n}"):
                taken = range(n * nz // CHUNKS, (n + 1) * nz // CHUNKS)
                mix_planes(peer, phase, middle + sign * nz, conj, True, taken)
        invert()

    with NS("zero"):
        zero_missing(0)
        zero_missing(1)
    with NS("wait_est"):
        load_est.wait()
    with NS("pack0"):
        do_pack(0, est_ref, pl.ds(0, nx))
    with NS("barrier"):
        if close:
            pl.semaphore_wait(barrier, beside_x + beside_y + beside_x * beside_y + 1)
        else:
            pl.semaphore_wait(barrier, everyone - 1)
    with NS("send0"):
        send_halo(0, est_ref, SIDES_Y)
        send_halo(0, est_ref, CORNERS)
        send_halo(0, est_ref, SIDES_X, pl.ds(0, nz))

    with NS("wait_loads"):
        load_index.wait()
        load_psf.wait()
        load_table.wait()
        load_view.wait()
    with NS("psf_prep"):
        chosen = psf[index_ref[0]]
        total = jnp.sum(chosen, axis=0)
        total = jnp.sum(jnp.sum(total, axis=1, keepdims=True), axis=0, keepdims=True)
        psf_pad[...] = jnp.zeros(psf_pad.shape, F32)
        psf_pad[pl.ds(0, extent), pl.ds(0, extent), pl.ds(0, extent)] = (
            chosen * (1.0 / total)[None]
        )

    with NS("prepare1"):

        @pl.loop(1, 3)
        def _(g):
            prepare(g * GROUP)

    def write_ratio(z, rows, blurred):
        ratio[z, rows, :] = view_ref[z, rows, :] / blurred

    def invert_blurred():
        for first, count in STEPS:
            with NS(f"inverse0_{first}"):
                inverse(range(first, first + count), (0,), write_ratio, keep=True)
                if first + count == nz:
                    for start, rows in segments[0]:
                        do_pack(1, ratio, pl.ds(start, rows))
                    send_halo(1, ratio, CORNERS)

                @pl.when(gz == 0)
                def _():
                    send_halo(1, ratio, SIDES_X, pl.ds(first, count))

        with NS("inverse0_middle"):
            inverse(range(nz), (1,), write_ratio, kept=True)
            @pl.when(gz == 1)
            def _():
                send_halo(1, ratio, SIDES_X, pl.ds(0, nz))

            for start, rows in segments[1]:
                do_pack(1, ratio, pl.ds(start, rows))
            send_halo(1, ratio, SIDES_Y)

    convolve(0, est_ref, False, invert_blurred)

    with NS("prepare3"):
        prepare(3 * GROUP * (1 - gz))
        cols5 = four_ref.shape[2] // 2
        i = lax.broadcasted_iota(jnp.int32, (LANES, LANES), 0)
        j = lax.broadcasted_iota(jnp.int32, (LANES, LANES), 1)
        target = i // (ny // cols5) + gy * cols5
        place5[...] = jnp.where(j == target, 1.0 / (nz * 2 * 32 * 32), 0.0).astype(BF)

    def write_update(z, rows, correction):
        out_ref[z, rows, :] = est_ref[z, rows, :] * correction

    def invert_correction():
        with NS("inverse1"):
            inverse(range(nz), (0, 1), write_update)

    convolve(1, ratio, True, invert_correction)

    with NS("five_send"):
        rows5 = four_ref.shape[1] // 2
        total = out_ref[0]
        for z in range(1, nz):
            total = total + out_ref[z]
        summed = jnp.sum(total.reshape(rows5, nx // rows5, ny), axis=1)
        hi, lo = split(summed)
        mine[...] = dot(hi, place5[...]) + dot(lo, place5[...])

        def slot(x, y, z):
            return (x * gyn + y) * 2 + z

        def send_tile(device):
            pltpu.make_async_remote_copy(
                src_ref=mine,
                dst_ref=tiles.at[slot(gx, gy, gz)],
                send_sem=gs,
                recv_sem=gr,
                device_id=device,
                device_id_type=MESH,
            ).start()

        for_others(send_tile)
        tiles[slot(gx, gy, gz)] = mine[...]

    def pooled(plane):
        hi, lo = split(plane)
        t = dot(hi, tab("py")) + dot(lo, tab("py"))
        hi, lo = split(t)
        return dot(tab("px"), hi) + dot(tab("px"), lo)

    with NS("pyramid"):
        halves = [(out_ref[2 * i] + out_ref[2 * i + 1]) * 0.5 for i in range(nz // 2)]
        quarters = [(halves[2 * i] + halves[2 * i + 1]) * 0.5 for i in range(nz // 4)]
        eighth = (quarters[0] + quarters[1]) * 0.5
        r4, c4 = places[3][0], places[3][2]
        last = pooled(eighth)
        share[0] = last[r4 : r4 + 8]
        share_copy = pltpu.make_async_remote_copy(
            src_ref=share.at[0], dst_ref=share_in, send_sem=ps, recv_sem=pr,
            device_id=partner, device_id_type=MESH,
        )
        share_copy.start()
        row, rows, col, cols = places[2]
        three_ref[0] = last[row : row + rows, col : col + cols]
        row, rows, col, cols = places[1]
        for i, plane in enumerate(quarters):
            two_ref[i] = pooled(plane)[row : row + rows, col : col + cols]
        row, rows, col, cols = places[0]
        for i, plane in enumerate(halves):
            one_ref[i] = pooled(plane)[row : row + rows, col : col + cols]
    with NS("share"):
        share_copy.wait()
        both = (share[0] + share_in[...]) * 0.5
        four_ref[0] = both[: places[3][1], c4 : c4 + places[3][3]]
    with NS("settle"):
        for phase in range(2):
            settle(hs.at[phase])
            pltpu.make_async_copy(own.at[phase], peer.at[phase], es.at[phase]).wait()
    with NS("wait_tiles"):
        others = tiles.at[pl.ds(0, everyone - 1)]
        pltpu.make_async_copy(others, others, gs).wait()
        pltpu.make_async_copy(others, others, gr).wait()
    with NS("five"):
        for x in range(gxn):
            five = tiles[slot(x, 0, 0)]
            for n in range(1, 2 * gyn):
                five = five + tiles[slot(x, 0, 0) + n]
            five_ref[0, pl.ds(x * rows5, rows5), :] = five[:, : five_ref.shape[2]]


def write_out(*refs):
    sems = refs[12]
    copies = [pltpu.make_async_copy(refs[i], refs[6 + i], sems.at[i]) for i in range(6)]
    for copy in copies:
        copy.start()
    for copy in copies:
        copy.wait()


def local(sizes, estimate, view_data, psf_stack, view_index):
    gxn, gyn = sizes
    nz, nx, ny = estimate.shape
    extent = psf_stack.shape[1]
    table, where, places = tables(nx, ny, extent)
    lx = nx + 2 * EDGE
    lp = 2 * (lx // 3)
    wide = extent + 1
    everyone = 2 * gxn * gyn
    vmem = pl.BlockSpec(memory_space=pltpu.VMEM)
    hbm = pl.BlockSpec(memory_space=pltpu.HBM)
    rows5, cols5 = nx // 32, ny // 32
    dma = pltpu.SemaphoreType.DMA
    shapes = (
        (nz, nx, ny),
        (nz // 2, nx // 2, ny // 2),
        (nz // 4, nx // 4, ny // 4),
        (nz // 8, nx // 8, ny // 8),
        (1, nx // 16, ny // 16),
        (1, rows5 * gxn, cols5 * gyn),
    )
    results = pl.pallas_call(
        functools.partial(kernel, sizes, where, places),
        out_shape=tuple(pltpu.VMEM(s, F32) for s in shapes),
        in_specs=[hbm] * 5,
        out_specs=(vmem,) * 6,
        scratch_shapes=[
            pltpu.SMEM(view_index.shape, view_index.dtype),
            pltpu.VMEM(estimate.shape, F32),
            pltpu.VMEM(view_data.shape, F32),
            pltpu.VMEM(psf_stack.shape, F32),
            pltpu.VMEM(table.shape, BF),
            pltpu.VMEM((wide, wide, LANES), F32),
            pltpu.VMEM((wide, 2 * lp, LANES), F32),
            pltpu.VMEM((2, nz, 2 * lp, LANES), F32),
            pltpu.VMEM((2, nz, 2 * lp, LANES), F32),
            pltpu.VMEM((nz, 2 * lx, LANES), F32),
            pltpu.VMEM((nz // 2, 2, 2 * lx, 2 * LANES), BF),
            pltpu.VMEM((nz, nx, ny), F32),
            pltpu.VMEM((2, 2, nx, LANES), F32),
            pltpu.VMEM((2, 2, nz, EDGE, ny), F32),
            pltpu.VMEM((2, 2, lx, LANES), F32),
            pltpu.VMEM((1, 8, LANES), F32),
            pltpu.VMEM((8, LANES), F32),
            pltpu.VMEM((LANES, LANES), BF),
            pltpu.VMEM((rows5, LANES), F32),
            pltpu.VMEM((everyone, rows5, LANES), F32),
            pltpu.VMEM((2 * nz * EDGE + 2 * nx + 4 * EDGE, LANES), F32),
            dma((5,)),
            dma((2,)),
            dma((2,)),
            dma((2,)),
            dma((2,)),
            dma((2, CHUNKS)),
            dma,
            dma,
            dma,
            dma,
        ],
        compiler_params=pltpu.CompilerParams(
            collective_id=0, has_side_effects=True, vmem_limit_bytes=48 * 1024 * 1024
        ),
        name="deconvolve",
    )(
        view_index,
        *[
            pltpu.with_memory_space_constraint(a, pltpu.HBM)
            for a in (estimate, view_data, psf_stack, jnp.asarray(table))
        ],
    )
    return pl.pallas_call(
        write_out,
        out_shape=tuple(jax.ShapeDtypeStruct(s, F32) for s in shapes),
        in_specs=[vmem] * 6,
        out_specs=(hbm,) * 6,
        scratch_shapes=[dma((6,))],
        name="write_out",
    )(*[pltpu.with_memory_space_constraint(r, pltpu.VMEM) for r in results])


def solution(mesh):
    return jax.shard_map(
        functools.partial(local, (mesh.shape["gx"], mesh.shape["gy"])),
        mesh=mesh,
        in_specs=(P("gz", "gx", "gy"), P("gz", "gx", "gy"), P(), P()),
        out_specs=(
            P("gz", "gx", "gy"),
            P("gz", "gx", "gy"),
            P("gz", "gx", "gy"),
            P("gz", "gx", "gy"),
            P(None, "gx", "gy"),
            P(),
        ),
        check_vma=False,
    )
```

```python
import functools
import math

import jax
import jax.numpy as jnp
import numpy as np
from jax import lax
from jax.experimental import pallas as pl
from jax.experimental.pallas import tpu as pltpu
from jax.sharding import PartitionSpec as P

MESH = pl.DeviceIdType.MESH
NS = jax.named_scope
BF = jnp.bfloat16
F32 = jnp.float32
LANES = 128
EDGE = 16
GROUP = 8
CHUNKS = 2
STEPS = ((0, 4), (4, 4))
CORNERS = ((1, 1), (-1, 1), (1, -1), (-1, -1))
SIDES_X = ((1, 0), (-1, 0))
SIDES_Y = ((0, 1), (0, -1))


def two_parts(matrix):
    matrix = np.asarray(matrix, np.float32)
    high = matrix.astype(BF)
    low = (matrix - high.astype(np.float32)).astype(BF)
    return high, low


def split(x):
    high = x.astype(BF)
    return high, (x - high.astype(F32)).astype(BF)


def dot(a, b):
    return jnp.dot(a, b, preferred_element_type=F32)


def tables(nx, ny, extent):
    radius = (extent - 1) // 2
    lx, ly = nx + 2 * EDGE, ny + 2 * EDGE
    nf = ly // 2 + 1
    wide = extent + 1
    freq_y = np.arange(nf)
    freq_x = np.arange(lx)

    def wave(k, n, length):
        return 2 * math.pi / length * np.mod(np.outer(k, n), length)

    pos = np.concatenate([EDGE + np.arange(ny), np.arange(EDGE), EDGE + ny + np.arange(EDGE)])
    fy = np.zeros((ny + 2 * EDGE, 2 * LANES))
    angle = wave(pos, freq_y, ly)
    fy[:, :nf] = np.cos(angle)
    fy[:, LANES : LANES + nf] = -np.sin(angle)
    ky = np.zeros((wide, 2 * LANES))
    angle = wave(np.arange(extent) - radius, freq_y, ly)
    ky[:extent, :nf] = np.cos(angle)
    ky[:extent, LANES : LANES + nf] = -np.sin(angle)
    iy = np.zeros((2 * LANES, ny))
    weight = np.full((nf, 1), 2.0)
    weight[0] = weight[-1] = 1.0
    angle = wave(freq_y, EDGE + np.arange(ny), ly)
    iy[:nf] = weight / ly * np.cos(angle)
    iy[LANES : LANES + nf] = -weight / ly * np.sin(angle)

    angle = wave(freq_x, np.arange(lx), lx)
    fx = np.block([[np.cos(angle), np.sin(angle)], [-np.sin(angle), np.cos(angle)]])
    angle = wave(EDGE + np.arange(nx), freq_x, lx)
    ix = np.block([[np.cos(angle), -np.sin(angle)], [np.sin(angle), np.cos(angle)]]) / lx
    kx = np.zeros((2 * lx, 2, wide))
    angle = wave(freq_x, np.arange(extent) - radius, lx)
    kx[:lx, 0, :extent] = np.cos(angle)
    kx[:lx, 1, :extent] = np.sin(angle)
    kx[lx:, 0, :extent] = -np.sin(angle)
    kx[lx:, 1, :extent] = np.cos(angle)
    kx = kx.reshape(2 * lx, 2 * wide)

    fy_hi, fy_lo = two_parts(fy)
    ky_hi, ky_lo = two_parts(ky)
    iy_hi, iy_lo = two_parts(iy)
    fx_hi, fx_lo = two_parts(fx)
    ix_hi, ix_lo = two_parts(ix)
    kx_hi, kx_lo = two_parts(kx)

    py = np.zeros((ny, LANES))
    px = np.zeros((nx, nx))
    row, col = 0, 0
    places = []
    for level in range(1, 5):
        size = 2**level
        rows, cols = nx // size, ny // size
        places.append((row, rows, col, cols))
        for r in range(rows):
            px[row + r, r * size : (r + 1) * size] = 1.0 / size
        for c in range(cols):
            py[c * size : (c + 1) * size, col + c] = 1.0 / size
        row, col = row + rows, col + cols

    inner = np.concatenate([EDGE + np.arange(nx), lx + EDGE + np.arange(nx)])
    outer = np.setdiff1d(np.arange(2 * lx), inner)
    x_edge = np.concatenate([np.arange(EDGE), nx - EDGE + np.arange(EDGE)])
    x_middle = EDGE + np.arange(nx - 2 * EDGE)
    inverse_rows = np.concatenate([x_edge, nx + x_edge, x_middle, nx + x_middle])
    blank = np.zeros((LANES - 3 * wide, 2 * LANES), BF)
    side_hi, side_lo = fy_hi[ny:], fy_lo[ny:]
    named = {
        "fya": np.concatenate([fy_hi[:ny], fy_hi[:ny]], 0),
        "fyb": np.concatenate([fy_lo[:ny], side_hi, side_hi, side_lo, blank], 0),
        "fxa": np.concatenate([fx_hi[:, inner], fx_hi[:, inner]], 1),
        "fxb": fx_lo[:, inner],
        "fxh": np.concatenate([fx_hi[:, outer], fx_hi[:, outer], fx_lo[:, outer]], 1),
        "ky3": np.concatenate([ky_hi, ky_hi, ky_lo, blank], 0),
        "kx3": np.concatenate([kx_hi, kx_hi, kx_lo], 1),
        "ix2": np.concatenate([part[inverse_rows] for part in (ix_hi, ix_lo)], 0),
        "iy2": np.concatenate([iy_hi, iy_lo], 1),
        "iy1": iy_hi,
        "py": py.astype(BF),
        "px": px.astype(BF),
    }
    stacked, where, row = [], {}, 0
    for name, a in named.items():
        rows, cols = a.shape
        where[name] = (row, rows, cols)
        full = np.zeros((rows, 2 * LANES), BF)
        full[:, :cols] = a
        stacked.append(full)
        row += rows
    return np.concatenate(stacked, 0), where, tuple(places)


def kernel(
    sizes, where, places,
    index_hbm, est_hbm, view_hbm, psf_hbm, table_hbm,
    out_ref, one_ref, two_ref, three_ref, four_ref, five_ref,
    index_ref, est_ref, view_ref, psf, table,
    psf_pad, k2, own, peer, mix, parts_of, ratio,
    pack, xhalo, yhalo, share, share_in, place5, mine, tiles, ruler,
    in_sem, hs, hx, hy, es, er, ps, pr, gs, gr,
):
    gxn, gyn = sizes
    nz, nx, ny = est_ref.shape
    extent = psf.shape[1]
    wide = extent + 1
    pairs = nz // 2
    lx = nx + 2 * EDGE
    nf = (ny + 2 * EDGE) // 2 + 1
    third = lx // 3
    lp = 2 * third
    half = (nf + 1) // 2
    middle = (extent - 1) // 2
    gx, gy, gz = lax.axis_index("gx"), lax.axis_index("gy"), lax.axis_index("gz")
    partner = {"gx": gx, "gy": gy, "gz": 1 - gz}
    chips = gxn * gyn
    everyone = 2 * chips

    def tab(name, first=0, count=None):
        row, rows, cols = where[name]
        return table[pl.ds(row + first, rows if count is None else count), pl.ds(0, cols)]

    load_est, load_index, load_psf, load_table, load_view = [
        pltpu.make_async_copy(a, b, in_sem.at[i])
        for i, (a, b) in enumerate(
            (
                (est_hbm, est_ref),
                (index_hbm, index_ref),
                (psf_hbm, psf),
                (table_hbm, table),
                (view_hbm, view_ref),
            )
        )
    ]
    load_est.start()

    def for_others(act):
        zs = (gz, 1 - gz)

        def column(x, ys, skip):
            for b, y in ys:
                for c in range(2):
                    if not (skip and b == 0 and c == 0):
                        act({"gx": x, "gy": y, "gz": zs[c]})

        order = (*range(1, gyn), 0)
        ys = [(b, lax.rem(gy + b, gyn)) for b in order]
        if gxn <= 4:
            for a in (*range(1, gxn), 0):
                column(lax.rem(gx + a, gxn), ys, a == 0)
        else:

            @pl.loop(1, gxn)
            def _(a):
                column(lax.rem(gx + a, gxn), ys, False)

            column(gx, ys, True)

    def signal(device):
        pl.semaphore_signal(barrier, inc=1, device_id=device, device_id_type=MESH)

    def exists(dx, dy):
        ok = None
        for c, n, d in ((gx, gxn, dx), (gy, gyn, dy)):
            if d > 0:
                t = c < n - 1
            elif d < 0:
                t = c > 0
            else:
                continue
            ok = t if ok is None else jnp.logical_and(ok, t)
        return ok

    beside_x = (gx > 0).astype(jnp.int32) + (gx < gxn - 1).astype(jnp.int32)
    beside_y = (gy > 0).astype(jnp.int32) + (gy < gyn - 1).astype(jnp.int32)

    barrier = pltpu.get_barrier_semaphore()
    close = max(gxn, gyn) <= 4
    if close:
        signal(partner)
        for dx, dy in SIDES_X + SIDES_Y + CORNERS:

            @pl.when(exists(dx, dy))
            def _():
                signal({"gx": gx + dx, "gy": gy + dy, "gz": gz})
    else:
        for_others(signal)
    load_psf.start()
    load_index.start()
    load_table.start()
    load_view.start()

    def halo_copy(phase, field, dx, dy, planes=None):
        if dy == 0:
            rows = slice(nx - EDGE, nx) if dx > 0 else slice(0, EDGE)
            source = field.at[planes, rows, :]
            target = xhalo.at[phase, 0 if dx > 0 else 1, planes]
        else:
            side = 0 if dy > 0 else 1
            if dx == 0:
                source, target = pack.at[phase, side], yhalo.at[phase, side, pl.ds(EDGE, nx), :]
            else:
                rows = pl.ds(nx - EDGE, EDGE) if dx > 0 else pl.ds(0, EDGE)
                to = pl.ds(0, EDGE) if dx > 0 else pl.ds(EDGE + nx, EDGE)
                source, target = pack.at[phase, side, rows, :], yhalo.at[phase, side, to, :]
        return pltpu.make_async_remote_copy(
            src_ref=source,
            dst_ref=target,
            send_sem=hs.at[phase],
            recv_sem=(hx if dx else hy).at[phase],
            device_id={"gx": gx + dx, "gy": gy + dy, "gz": gz},
            device_id_type=MESH,
        )

    def send_halo(phase, field, directions, planes=None):
        def send(dx, dy, condition=True):
            @pl.when(jnp.logical_and(exists(dx, dy), condition))
            def _():
                halo_copy(phase, field, dx, dy, planes).start()

        odd = lax.rem(gx, 2) == 1
        for dx, dy in directions:
            if dx:
                send(dx, dy, odd if dx > 0 else jnp.logical_not(odd))
        for dx, dy in directions:
            if dx:
                send(dx, dy, odd if dx < 0 else jnp.logical_not(odd))
            else:
                send(dx, dy)

    def settle(sem, along_x=True, along_y=True):
        for a in range(3):
            for b in range(3):
                rows = (nz * EDGE * a + EDGE * a * b) * along_x + nx * b * along_y
                if rows:

                    @pl.when(jnp.logical_and(beside_x == a, beside_y == b))
                    def _():
                        part = ruler.at[pl.ds(0, rows)]
                        pltpu.make_async_copy(part, part, sem).wait()

    def do_pack(phase, field, rows):
        count = rows.size
        lane = lax.broadcasted_iota(jnp.int32, (count, LANES), 1) // EDGE
        for side in range(2):
            packed = jnp.zeros((count, LANES), F32)
            for z in range(nz):
                shift = (EDGE * z + EDGE * (1 - side)) % LANES
                cells = field[z, rows, :]
                packed = jnp.where(lane == z, pltpu.roll(cells, shift, 1) if shift else cells, packed)
            pack[phase, side, rows, :] = packed

    def zero_missing(phase):
        for dx, dy in SIDES_X + SIDES_Y + CORNERS:
            if dy == 0:
                target = xhalo.at[phase, 0 if dx > 0 else 1]
            else:
                side = 0 if dy > 0 else 1
                first, count = {0: (EDGE, nx), 1: (0, EDGE), -1: (EDGE + nx, EDGE)}[dx]
                target = yhalo.at[phase, side, pl.ds(first, count), :]

            @pl.when(jnp.logical_not(exists(-dx, -dy)))
            def _():
                target[...] = jnp.zeros(target.shape, F32)

    def swap_copy(phase, n):
        planes = pl.ds(n * nz // CHUNKS, nz // CHUNKS)
        return pltpu.make_async_remote_copy(
            src_ref=own.at[phase, planes],
            dst_ref=peer.at[phase, planes],
            send_sem=es.at[phase],
            recv_sem=er.at[phase, n],
            device_id=partner,
            device_id_type=MESH,
        )

    def fold(x):
        lane = lax.broadcasted_iota(jnp.int32, (lp, LANES), 1)
        rest = x[lp:lx]
        beside = jnp.concatenate(
            [pltpu.roll(rest, nf, 1), pltpu.roll(rest, nf - half, 1)], axis=0
        )
        return jnp.where(lane < nf, x[:lp], beside)

    def unfold(x):
        lane = lax.broadcasted_iota(jnp.int32, (third, LANES), 1)
        low = pltpu.roll(x[:third], LANES - nf, 1)
        high = pltpu.roll(x[third:lp], LANES - (nf - half), 1)
        return jnp.concatenate([x[:lp], jnp.where(lane < half, low, high)], axis=0)

    def beside(phase, z, first, count):
        lane = lax.broadcasted_iota(jnp.int32, (count, LANES), 1)
        left, right = (yhalo[phase, side, pl.ds(first, count), :] for side in range(2))
        if z:
            left = pltpu.roll(left, LANES - EDGE * z, 1)
        if z != 1:
            right = pltpu.roll(right, (EDGE - EDGE * z) % LANES, 1)
        side = jnp.where(lane < EDGE, left, jnp.where(lane < 2 * EDGE, right, 0.0))
        high = side.astype(BF).astype(F32)
        low = side - high
        return (high + pltpu.roll(low, 2 * EDGE, 1) + pltpu.roll(high, 4 * EDGE, 1)).astype(BF)

    def along_y(rows, sides):
        count = len(rows)
        hi, lo = split(jnp.concatenate([jnp.concatenate(r, axis=0) for r in rows], axis=0))
        side = jnp.concatenate([jnp.concatenate(r, axis=0) for r in sides], axis=0)
        x1 = dot(jnp.concatenate([hi, lo], axis=1), tab("fya")) + dot(
            jnp.concatenate([hi, side], axis=1), tab("fyb")
        )
        n = x1.shape[0] // count
        stacked = [
            jnp.concatenate([x1[k * n : (k + 1) * n, :LANES], x1[k * n : (k + 1) * n, LANES:]], 0)
            for k in range(count)
        ]
        return [split(jnp.concatenate(stacked[k : k + 2], axis=1)) for k in range(0, count, 2)]

    def forward(phase, field, planes):
        spectra = along_y(
            [[field[z]] for z in planes], [[beside(phase, z, EDGE, nx)] for z in planes]
        )
        for q, (hi, lo) in enumerate(spectra):
            x2 = dot(tab("fxa"), jnp.concatenate([hi, lo], axis=0)) + dot(tab("fxb"), hi)
            for k in range(2):
                z = planes[2 * q + k]
                part = x2[:, k * LANES : (k + 1) * LANES]
                mix[z] = part

    def forward_edges(phase, planes):
        spectra = along_y(
            [[xhalo[phase, side, z] for side in range(2)] for z in planes],
            [[beside(phase, z, first, EDGE) for first in (0, EDGE + nx)] for z in planes],
        )
        for q, (hi, lo) in enumerate(spectra):
            x2 = dot(tab("fxh"), jnp.concatenate([hi, lo, hi], axis=0))
            for k in range(2):
                z = planes[2 * q + k]
                part = mix[z] + x2[:, k * LANES : (k + 1) * LANES]
                own[phase, z, pl.ds(0, lp), :] = fold(part[:lx])
                own[phase, z, pl.ds(lp, lp), :] = fold(part[lx:])

    def mix_planes(source, phase, base, conj, add, taken):
        @pl.loop(0, lp // 8)
        def _(s):
            re = pl.ds(pl.multiple_of(s * 8, 8), 8)
            im = pl.ds(pl.multiple_of(lp + s * 8, 8), 8)
            vr = {j: source[phase, j, re, :] for j in taken}
            vi = {j: source[phase, j, im, :] for j in taken}
            kr, ki = {}, {}
            for d in sorted({j - i if conj else i - j for i in range(nz) for j in taken}):
                kr[d] = k2[base + d, re, :]
                ki[d] = k2[base + d, im, :]
            ks = {d: kr[d] - ki[d] if conj else kr[d] + ki[d] for d in kr}
            vs = {j: vr[j] + vi[j] for j in taken}
            for i in range(nz):
                a = b = c = None
                for j in taken:
                    d = j - i if conj else i - j
                    rr, ii, ss = kr[d] * vr[j], ki[d] * vi[j], ks[d] * vs[j]
                    a = rr if a is None else a + rr
                    b = ii if b is None else b + ii
                    c = ss if c is None else c + ss
                yr = a + b if conj else a - b
                yi = c - a + b if conj else c - a - b
                mix[i, re, :] = mix[i, re, :] + yr if add else yr
                mix[i, im, :] = mix[i, im, :] + yi if add else yi

    segments = (((0, EDGE), (nx - EDGE, EDGE)), ((EDGE, nx - 2 * EDGE),))

    def unfolded(z):
        return jnp.concatenate([unfold(mix[z, pl.ds(0, lp)]), unfold(mix[z, pl.ds(lp, lp)])], 0)

    def inverse(planes, parts, write, keep=False, kept=False):
        counts = [sum(count for _, count in segments[p]) for p in parts]
        offset = 2 * sum(count for _, count in segments[0]) * parts[0]
        rows = []
        for z in planes[::2]:
            if kept:
                hi, lo = parts_of[z // 2, 0], parts_of[z // 2, 1]
            else:
                hi, lo = split(jnp.concatenate([unfolded(z), unfolded(z + 1)], axis=1))
            if keep:
                parts_of[z // 2, 0] = hi
                parts_of[z // 2, 1] = lo
            high = tab("ix2", offset, 2 * sum(counts))
            g = dot(high, hi) + dot(tab("ix2", 2 * nx + offset, 2 * sum(counts)), hi) + dot(high, lo)
            for k in range(2):
                part = g[:, k * LANES : (k + 1) * LANES]
                for count in counts:
                    rows.append(jnp.concatenate([part[:count], part[count : 2 * count]], axis=1))
                    part = part[2 * count :]
        hi, lo = split(jnp.concatenate(rows, axis=0))
        both = dot(hi, tab("iy2"))
        values = both[:, :ny] + both[:, ny:] + dot(lo, tab("iy1"))
        row = 0
        for z in planes:
            for p in parts:
                for first, count in segments[p]:
                    write(z, pl.ds(first, count), values[row : row + count])
                    row += count

    def prepare(first):
        block = psf_pad[pl.ds(first, GROUP)].reshape(GROUP * wide, LANES)
        high = block.astype(BF).astype(F32)
        low = block - high
        x1 = dot(
            (high + pltpu.roll(low, wide, 1) + pltpu.roll(high, 2 * wide, 1)).astype(BF),
            tab("ky3"),
        )
        hi, lo = split(x1)
        hi = hi.reshape(GROUP, wide, 2 * LANES)
        lo = lo.reshape(GROUP, wide, 2 * LANES)
        for h in range(GROUP // 2):
            columns = []
            for n in (2 * h, 2 * h + 1):
                parts = []
                for part in (hi[n], lo[n], hi[n]):
                    parts.append(part[:, :LANES])
                    parts.append(part[:, LANES:])
                columns.append(jnp.concatenate(parts, axis=0))
            spectrum = dot(tab("kx3"), jnp.concatenate(columns, axis=1))
            for n in range(2):
                part = spectrum[:, n * LANES : (n + 1) * LANES]
                k2[first + 2 * h + n, pl.ds(0, lp), :] = fold(part[:lx])
                k2[first + 2 * h + n, pl.ds(lp, lp), :] = fold(part[lx:])

    def convolve(phase, field, conj, invert):
        with NS(f"wait_haloy{phase}"):
            settle(hy.at[phase], along_x=False)
        with NS(f"forward{phase}"):
            for z in range(0, nz, 8):
                forward(phase, field, range(z, z + 8))
        if phase == 0:
            with NS("prepare2"):
                prepare(3 * GROUP * gz)
        with NS(f"wait_halox{phase}"):
            settle(hx.at[phase], along_y=False)
        with NS(f"edges{phase}"):
            forward_edges(phase, range(nz))
            for n in range(CHUNKS):
                swap_copy(phase, n).start()
        sign = 1 - 2 * gz if conj else 2 * gz - 1
        with NS(f"mixown{phase}"):
            mix_planes(own, phase, middle, conj, False, range(nz))
        for n in range(CHUNKS):
            with NS(f"waitswap{phase}_{n}"):
                swap_copy(phase, n).wait_recv()
            with NS(f"mixpeer{phase}_{n}"):
                taken = range(n * nz // CHUNKS, (n + 1) * nz // CHUNKS)
                mix_planes(peer, phase, middle + sign * nz, conj, True, taken)
        invert()

    with NS("zero"):
        zero_missing(0)
        zero_missing(1)
    with NS("wait_est"):
        load_est.wait()
    with NS("pack0"):
        do_pack(0, est_ref, pl.ds(0, nx))
    with NS("barrier"):
        if close:
            pl.semaphore_wait(barrier, beside_x + beside_y + beside_x * beside_y + 1)
        else:
            pl.semaphore_wait(barrier, everyone - 1)
    with NS("send0"):
        send_halo(0, est_ref, SIDES_Y)
        send_halo(0, est_ref, CORNERS)
        send_halo(0, est_ref, SIDES_X, pl.ds(0, nz))

    with NS("wait_loads"):
        load_index.wait()
        load_psf.wait()
        load_table.wait()
        load_view.wait()
    with NS("psf_prep"):
        chosen = psf[index_ref[0]]
        total = jnp.sum(chosen, axis=0)
        total = jnp.sum(jnp.sum(total, axis=1, keepdims=True), axis=0, keepdims=True)
        psf_pad[...] = jnp.zeros(psf_pad.shape, F32)
        psf_pad[pl.ds(0, extent), pl.ds(0, extent), pl.ds(0, extent)] = (
            chosen * (1.0 / total)[None]
        )

    with NS("prepare1"):

        @pl.loop(1, 3)
        def _(g):
            prepare(g * GROUP)

    def write_ratio(z, rows, blurred):
        ratio[z, rows, :] = view_ref[z, rows, :] / blurred

    def invert_blurred():
        for first, count in STEPS:
            with NS(f"inverse0_{first}"):
                inverse(range(first, first + count), (0,), write_ratio, keep=True)
                if first + count == nz:
                    for start, rows in segments[0]:
                        do_pack(1, ratio, pl.ds(start, rows))
                    send_halo(1, ratio, CORNERS)

                @pl.when(gz == 0)
                def _():
                    send_halo(1, ratio, SIDES_X, pl.ds(first, count))

                if first:

                    @pl.when(gz == 1)
                    def _():
                        send_halo(1, ratio, SIDES_X, pl.ds(0, first))

        with NS("inverse0_middle"):
            inverse(range(nz), (1,), write_ratio, kept=True)
            @pl.when(gz == 1)
            def _():
                send_halo(1, ratio, SIDES_X, pl.ds(*STEPS[-1]))

            for start, rows in segments[1]:
                do_pack(1, ratio, pl.ds(start, rows))
            send_halo(1, ratio, SIDES_Y)

    convolve(0, est_ref, False, invert_blurred)

    with NS("prepare3"):
        prepare(3 * GROUP * (1 - gz))
        cols5 = four_ref.shape[2] // 2
        i = lax.broadcasted_iota(jnp.int32, (LANES, LANES), 0)
        j = lax.broadcasted_iota(jnp.int32, (LANES, LANES), 1)
        target = i // (ny // cols5) + gy * cols5
        place5[...] = jnp.where(j == target, 1.0 / (nz * 2 * 32 * 32), 0.0).astype(BF)

    def write_update(z, rows, correction):
        out_ref[z, rows, :] = est_ref[z, rows, :] * correction

    def invert_correction():
        with NS("inverse1"):
            inverse(range(nz), (0, 1), write_update)

    convolve(1, ratio, True, invert_correction)

    with NS("five_send"):
        rows5 = four_ref.shape[1] // 2
        total = out_ref[0]
        for z in range(1, nz):
            total = total + out_ref[z]
        summed = jnp.sum(total.reshape(rows5, nx // rows5, ny), axis=1)
        hi, lo = split(summed)
        mine[...] = dot(hi, place5[...]) + dot(lo, place5[...])

        def slot(x, y, z):
            return (x * gyn + y) * 2 + z

        def send_tile(device):
            pltpu.make_async_remote_copy(
                src_ref=mine,
                dst_ref=tiles.at[slot(gx, gy, gz)],
                send_sem=gs,
                recv_sem=gr,
                device_id=device,
                device_id_type=MESH,
            ).start()

        for_others(send_tile)
        tiles[slot(gx, gy, gz)] = mine[...]

    def pooled(plane):
        hi, lo = split(plane)
        t = dot(hi, tab("py")) + dot(lo, tab("py"))
        hi, lo = split(t)
        return dot(tab("px"), hi) + dot(tab("px"), lo)

    with NS("pyramid"):
        halves = [(out_ref[2 * i] + out_ref[2 * i + 1]) * 0.5 for i in range(nz // 2)]
        quarters = [(halves[2 * i] + halves[2 * i + 1]) * 0.5 for i in range(nz // 4)]
        eighth = (quarters[0] + quarters[1]) * 0.5
        r4, c4 = places[3][0], places[3][2]
        last = pooled(eighth)
        share[0] = last[r4 : r4 + 8]
        share_copy = pltpu.make_async_remote_copy(
            src_ref=share.at[0], dst_ref=share_in, send_sem=ps, recv_sem=pr,
            device_id=partner, device_id_type=MESH,
        )
        share_copy.start()
        row, rows, col, cols = places[2]
        three_ref[0] = last[row : row + rows, col : col + cols]
        row, rows, col, cols = places[1]
        for i, plane in enumerate(quarters):
            two_ref[i] = pooled(plane)[row : row + rows, col : col + cols]
        row, rows, col, cols = places[0]
        for i, plane in enumerate(halves):
            one_ref[i] = pooled(plane)[row : row + rows, col : col + cols]
    with NS("share"):
        share_copy.wait()
        both = (share[0] + share_in[...]) * 0.5
        four_ref[0] = both[: places[3][1], c4 : c4 + places[3][3]]
    with NS("settle"):
        for phase in range(2):
            settle(hs.at[phase])
            pltpu.make_async_copy(own.at[phase], peer.at[phase], es.at[phase]).wait()
    with NS("wait_tiles"):
        others = tiles.at[pl.ds(0, everyone - 1)]
        pltpu.make_async_copy(others, others, gs).wait()
        pltpu.make_async_copy(others, others, gr).wait()
    with NS("five"):
        for x in range(gxn):
            five = tiles[slot(x, 0, 0)]
            for n in range(1, 2 * gyn):
                five = five + tiles[slot(x, 0, 0) + n]
            five_ref[0, pl.ds(x * rows5, rows5), :] = five[:, : five_ref.shape[2]]


def write_out(*refs):
    sems = refs[12]
    copies = [pltpu.make_async_copy(refs[i], refs[6 + i], sems.at[i]) for i in range(6)]
    for copy in copies:
        copy.start()
    for copy in copies:
        copy.wait()


def local(sizes, estimate, view_data, psf_stack, view_index):
    gxn, gyn = sizes
    nz, nx, ny = estimate.shape
    extent = psf_stack.shape[1]
    table, where, places = tables(nx, ny, extent)
    lx = nx + 2 * EDGE
    lp = 2 * (lx // 3)
    wide = extent + 1
    everyone = 2 * gxn * gyn
    vmem = pl.BlockSpec(memory_space=pltpu.VMEM)
    hbm = pl.BlockSpec(memory_space=pltpu.HBM)
    rows5, cols5 = nx // 32, ny // 32
    dma = pltpu.SemaphoreType.DMA
    shapes = (
        (nz, nx, ny),
        (nz // 2, nx // 2, ny // 2),
        (nz // 4, nx // 4, ny // 4),
        (nz // 8, nx // 8, ny // 8),
        (1, nx // 16, ny // 16),
        (1, rows5 * gxn, cols5 * gyn),
    )
    results = pl.pallas_call(
        functools.partial(kernel, sizes, where, places),
        out_shape=tuple(pltpu.VMEM(s, F32) for s in shapes),
        in_specs=[hbm] * 5,
        out_specs=(vmem,) * 6,
        scratch_shapes=[
            pltpu.SMEM(view_index.shape, view_index.dtype),
            pltpu.VMEM(estimate.shape, F32),
            pltpu.VMEM(view_data.shape, F32),
            pltpu.VMEM(psf_stack.shape, F32),
            pltpu.VMEM(table.shape, BF),
            pltpu.VMEM((wide, wide, LANES), F32),
            pltpu.VMEM((wide, 2 * lp, LANES), F32),
            pltpu.VMEM((2, nz, 2 * lp, LANES), F32),
            pltpu.VMEM((2, nz, 2 * lp, LANES), F32),
            pltpu.VMEM((nz, 2 * lx, LANES), F32),
            pltpu.VMEM((nz // 2, 2, 2 * lx, 2 * LANES), BF),
            pltpu.VMEM((nz, nx, ny), F32),
            pltpu.VMEM((2, 2, nx, LANES), F32),
            pltpu.VMEM((2, 2, nz, EDGE, ny), F32),
            pltpu.VMEM((2, 2, lx, LANES), F32),
            pltpu.VMEM((1, 8, LANES), F32),
            pltpu.VMEM((8, LANES), F32),
            pltpu.VMEM((LANES, LANES), BF),
            pltpu.VMEM((rows5, LANES), F32),
            pltpu.VMEM((everyone, rows5, LANES), F32),
            pltpu.VMEM((2 * nz * EDGE + 2 * nx + 4 * EDGE, LANES), F32),
            dma((5,)),
            dma((2,)),
            dma((2,)),
            dma((2,)),
            dma((2,)),
            dma((2, CHUNKS)),
            dma,
            dma,
            dma,
            dma,
        ],
        compiler_params=pltpu.CompilerParams(
            collective_id=0, has_side_effects=True, vmem_limit_bytes=48 * 1024 * 1024
        ),
        name="deconvolve",
    )(
        view_index,
        *[
            pltpu.with_memory_space_constraint(a, pltpu.HBM)
            for a in (estimate, view_data, psf_stack, jnp.asarray(table))
        ],
    )
    return pl.pallas_call(
        write_out,
        out_shape=tuple(jax.ShapeDtypeStruct(s, F32) for s in shapes),
        in_specs=[vmem] * 6,
        out_specs=(hbm,) * 6,
        scratch_shapes=[dma((6,))],
        name="write_out",
    )(*[pltpu.with_memory_space_constraint(r, pltpu.VMEM) for r in results])


def solution(mesh):
    return jax.shard_map(
        functools.partial(local, (mesh.shape["gx"], mesh.shape["gy"])),
        mesh=mesh,
        in_specs=(P("gz", "gx", "gy"), P("gz", "gx", "gy"), P(), P()),
        out_specs=(
            P("gz", "gx", "gy"),
            P("gz", "gx", "gy"),
            P("gz", "gx", "gy"),
            P("gz", "gx", "gy"),
            P(None, "gx", "gy"),
            P(),
        ),
        check_vma=False,
    )
```

```python
import functools
import math

import jax
import jax.numpy as jnp
import numpy as np
from jax import lax
from jax.experimental import pallas as pl
from jax.experimental.pallas import tpu as pltpu
from jax.sharding import PartitionSpec as P

MESH = pl.DeviceIdType.MESH
NS = jax.named_scope
BF = jnp.bfloat16
F32 = jnp.float32
LANES = 128
EDGE = 16
GROUP = 8
CHUNKS = 2
STEPS = ((0, 4), (4, 4))
CORNERS = ((1, 1), (-1, 1), (1, -1), (-1, -1))
SIDES_X = ((1, 0), (-1, 0))
SIDES_Y = ((0, 1), (0, -1))


def two_parts(matrix):
    matrix = np.asarray(matrix, np.float32)
    high = matrix.astype(BF)
    low = (matrix - high.astype(np.float32)).astype(BF)
    return high, low


def split(x):
    high = x.astype(BF)
    return high, (x - high.astype(F32)).astype(BF)


def dot(a, b):
    return jnp.dot(a, b, preferred_element_type=F32)


def tables(nx, ny, extent):
    radius = (extent - 1) // 2
    lx, ly = nx + 2 * EDGE, ny + 2 * EDGE
    nf = ly // 2 + 1
    wide = extent + 1
    freq_y = np.arange(nf)
    freq_x = np.arange(lx)

    def wave(k, n, length):
        return 2 * math.pi / length * np.mod(np.outer(k, n), length)

    pos = np.concatenate([EDGE + np.arange(ny), np.arange(EDGE), EDGE + ny + np.arange(EDGE)])
    fy = np.zeros((ny + 2 * EDGE, 2 * LANES))
    angle = wave(pos, freq_y, ly)
    fy[:, :nf] = np.cos(angle)
    fy[:, LANES : LANES + nf] = -np.sin(angle)
    ky = np.zeros((wide, 2 * LANES))
    angle = wave(np.arange(extent) - radius, freq_y, ly)
    ky[:extent, :nf] = np.cos(angle)
    ky[:extent, LANES : LANES + nf] = -np.sin(angle)
    iy = np.zeros((2 * LANES, ny))
    weight = np.full((nf, 1), 2.0)
    weight[0] = weight[-1] = 1.0
    angle = wave(freq_y, EDGE + np.arange(ny), ly)
    iy[:nf] = weight / ly * np.cos(angle)
    iy[LANES : LANES + nf] = -weight / ly * np.sin(angle)

    angle = wave(freq_x, np.arange(lx), lx)
    fx = np.block([[np.cos(angle), np.sin(angle)], [-np.sin(angle), np.cos(angle)]])
    angle = wave(EDGE + np.arange(nx), freq_x, lx)
    ix = np.block([[np.cos(angle), -np.sin(angle)], [np.sin(angle), np.cos(angle)]]) / lx
    kx = np.zeros((2 * lx, 2, wide))
    angle = wave(freq_x, np.arange(extent) - radius, lx)
    kx[:lx, 0, :extent] = np.cos(angle)
    kx[:lx, 1, :extent] = np.sin(angle)
    kx[lx:, 0, :extent] = -np.sin(angle)
    kx[lx:, 1, :extent] = np.cos(angle)
    kx = kx.reshape(2 * lx, 2 * wide)

    fy_hi, fy_lo = two_parts(fy)
    ky_hi, ky_lo = two_parts(ky)
    iy_hi, iy_lo = two_parts(iy)
    fx_hi, fx_lo = two_parts(fx)
    ix_hi, ix_lo = two_parts(ix)
    kx_hi, kx_lo = two_parts(kx)

    py = np.zeros((ny, LANES))
    px = np.zeros((nx, nx))
    row, col = 0, 0
    places = []
    for level in range(1, 5):
        size = 2**level
        rows, cols = nx // size, ny // size
        places.append((row, rows, col, cols))
        for r in range(rows):
            px[row + r, r * size : (r + 1) * size] = 1.0 / size
        for c in range(cols):
            py[c * size : (c + 1) * size, col + c] = 1.0 / size
        row, col = row + rows, col + cols

    inner = np.concatenate([EDGE + np.arange(nx), lx + EDGE + np.arange(nx)])
    outer = np.setdiff1d(np.arange(2 * lx), inner)
    x_edge = np.concatenate([np.arange(EDGE), nx - EDGE + np.arange(EDGE)])
    x_middle = EDGE + np.arange(nx - 2 * EDGE)
    inverse_rows = np.concatenate([x_edge, nx + x_edge, x_middle, nx + x_middle])
    blank = np.zeros((LANES - 3 * wide, 2 * LANES), BF)
    side_hi, side_lo = fy_hi[ny:], fy_lo[ny:]
    named = {
        "fya": np.concatenate([fy_hi[:ny], fy_hi[:ny]], 0),
        "fyb": np.concatenate([fy_lo[:ny], side_hi, side_hi, side_lo, blank], 0),
        "fxa": np.concatenate([fx_hi[:, inner], fx_hi[:, inner]], 1),
        "fxb": fx_lo[:, inner],
        "fxh": np.concatenate([fx_hi[:, outer], fx_hi[:, outer], fx_lo[:, outer]], 1),
        "ky3": np.concatenate([ky_hi, ky_hi, ky_lo, blank], 0),
        "kx3": np.concatenate([kx_hi, kx_hi, kx_lo], 1),
        "ix2": np.concatenate([part[inverse_rows] for part in (ix_hi, ix_lo)], 0),
        "iy2": np.concatenate([iy_hi, iy_lo], 1),
        "iy1": iy_hi,
        "py": py.astype(BF),
        "px": px.astype(BF),
    }
    stacked, where, row = [], {}, 0
    for name, a in named.items():
        rows, cols = a.shape
        where[name] = (row, rows, cols)
        full = np.zeros((rows, 2 * LANES), BF)
        full[:, :cols] = a
        stacked.append(full)
        row += rows
    return np.concatenate(stacked, 0), where, tuple(places)


def kernel(
    sizes, where, places,
    index_hbm, est_hbm, view_hbm, psf_hbm, table_hbm,
    out_ref, one_ref, two_ref, three_ref, four_ref, five_ref,
    index_ref, est_ref, view_ref, psf, table,
    psf_pad, k2, own, peer, mix, parts_of, ratio,
    pack, xhalo, yhalo, share, share_in, place5, mine, tiles, ruler,
    in_sem, hs, hx, hy, es, er, ps, pr, gs, gr,
):
    gxn, gyn = sizes
    nz, nx, ny = est_ref.shape
    extent = psf.shape[1]
    wide = extent + 1
    pairs = nz // 2
    lx = nx + 2 * EDGE
    nf = (ny + 2 * EDGE) // 2 + 1
    third = lx // 3
    lp = 2 * third
    half = (nf + 1) // 2
    middle = (extent - 1) // 2
    gx, gy, gz = lax.axis_index("gx"), lax.axis_index("gy"), lax.axis_index("gz")
    partner = {"gx": gx, "gy": gy, "gz": 1 - gz}
    chips = gxn * gyn
    everyone = 2 * chips

    def tab(name, first=0, count=None):
        row, rows, cols = where[name]
        return table[pl.ds(row + first, rows if count is None else count), pl.ds(0, cols)]

    load_est, load_index, load_psf, load_table, load_view = [
        pltpu.make_async_copy(a, b, in_sem.at[i])
        for i, (a, b) in enumerate(
            (
                (est_hbm, est_ref),
                (index_hbm, index_ref),
                (psf_hbm, psf),
                (table_hbm, table),
                (view_hbm, view_ref),
            )
        )
    ]
    load_est.start()

    def for_others(act):
        zs = (gz, 1 - gz)

        def column(x, ys, skip):
            for b, y in ys:
                for c in range(2):
                    if not (skip and b == 0 and c == 0):
                        act({"gx": x, "gy": y, "gz": zs[c]})

        order = (*range(1, gyn), 0)
        ys = [(b, lax.rem(gy + b, gyn)) for b in order]
        if gxn <= 4:
            for a in (*range(1, gxn), 0):
                column(lax.rem(gx + a, gxn), ys, a == 0)
        else:

            @pl.loop(1, gxn)
            def _(a):
                column(lax.rem(gx + a, gxn), ys, False)

            column(gx, ys, True)

    def signal(device):
        pl.semaphore_signal(barrier, inc=1, device_id=device, device_id_type=MESH)

    def exists(dx, dy):
        ok = None
        for c, n, d in ((gx, gxn, dx), (gy, gyn, dy)):
            if d > 0:
                t = c < n - 1
            elif d < 0:
                t = c > 0
            else:
                continue
            ok = t if ok is None else jnp.logical_and(ok, t)
        return ok

    beside_x = (gx > 0).astype(jnp.int32) + (gx < gxn - 1).astype(jnp.int32)
    beside_y = (gy > 0).astype(jnp.int32) + (gy < gyn - 1).astype(jnp.int32)

    barrier = pltpu.get_barrier_semaphore()
    close = max(gxn, gyn) <= 4
    if close:
        signal(partner)
        for dx, dy in SIDES_X + SIDES_Y + CORNERS:

            @pl.when(exists(dx, dy))
            def _():
                signal({"gx": gx + dx, "gy": gy + dy, "gz": gz})
    else:
        for_others(signal)
    load_psf.start()
    load_index.start()
    load_table.start()
    load_view.start()

    def halo_copy(phase, field, dx, dy, planes=None):
        if dy == 0:
            rows = slice(nx - EDGE, nx) if dx > 0 else slice(0, EDGE)
            source = field.at[planes, rows, :]
            target = xhalo.at[phase, 0 if dx > 0 else 1, planes]
        else:
            side = 0 if dy > 0 else 1
            if dx == 0:
                source, target = pack.at[phase, side], yhalo.at[phase, side, pl.ds(EDGE, nx), :]
            else:
                rows = pl.ds(nx - EDGE, EDGE) if dx > 0 else pl.ds(0, EDGE)
                to = pl.ds(0, EDGE) if dx > 0 else pl.ds(EDGE + nx, EDGE)
                source, target = pack.at[phase, side, rows, :], yhalo.at[phase, side, to, :]
        return pltpu.make_async_remote_copy(
            src_ref=source,
            dst_ref=target,
            send_sem=hs.at[phase],
            recv_sem=(hx if dx else hy).at[phase],
            device_id={"gx": gx + dx, "gy": gy + dy, "gz": gz},
            device_id_type=MESH,
        )

    def send_halo(phase, field, directions, planes=None):
        def send(dx, dy, condition=True):
            @pl.when(jnp.logical_and(exists(dx, dy), condition))
            def _():
                halo_copy(phase, field, dx, dy, planes).start()

        odd = lax.rem(gx, 2) == 1
        for dx, dy in directions:
            if dx:
                send(dx, dy, odd if dx > 0 else jnp.logical_not(odd))
        for dx, dy in directions:
            if dx:
                send(dx, dy, odd if dx < 0 else jnp.logical_not(odd))
            else:
                send(dx, dy)

    def settle(sem, along_x=True, along_y=True):
        for a in range(3):
            for b in range(3):
                rows = (nz * EDGE * a + EDGE * a * b) * along_x + nx * b * along_y
                if rows:

                    @pl.when(jnp.logical_and(beside_x == a, beside_y == b))
                    def _():
                        part = ruler.at[pl.ds(0, rows)]
                        pltpu.make_async_copy(part, part, sem).wait()

    def do_pack(phase, field, rows):
        count = rows.size
        lane = lax.broadcasted_iota(jnp.int32, (count, LANES), 1) // EDGE
        for side in range(2):
            packed = jnp.zeros((count, LANES), F32)
            for z in range(nz):
                shift = (EDGE * z + EDGE * (1 - side)) % LANES
                cells = field[z, rows, :]
                packed = jnp.where(lane == z, pltpu.roll(cells, shift, 1) if shift else cells, packed)
            pack[phase, side, rows, :] = packed

    def zero_missing(phase):
        for dx, dy in SIDES_X + SIDES_Y + CORNERS:
            if dy == 0:
                target = xhalo.at[phase, 0 if dx > 0 else 1]
            else:
                side = 0 if dy > 0 else 1
                first, count = {0: (EDGE, nx), 1: (0, EDGE), -1: (EDGE + nx, EDGE)}[dx]
                target = yhalo.at[phase, side, pl.ds(first, count), :]

            @pl.when(jnp.logical_not(exists(-dx, -dy)))
            def _():
                target[...] = jnp.zeros(target.shape, F32)

    def swap_copy(phase, n):
        planes = pl.ds(n * nz // CHUNKS, nz // CHUNKS)
        return pltpu.make_async_remote_copy(
            src_ref=own.at[phase, planes],
            dst_ref=peer.at[phase, planes],
            send_sem=es.at[phase],
            recv_sem=er.at[phase, n],
            device_id=partner,
            device_id_type=MESH,
        )

    def fold(x):
        lane = lax.broadcasted_iota(jnp.int32, (lp, LANES), 1)
        rest = x[lp:lx]
        beside = jnp.concatenate(
            [pltpu.roll(rest, nf, 1), pltpu.roll(rest, nf - half, 1)], axis=0
        )
        return jnp.where(lane < nf, x[:lp], beside)

    def unfold(x):
        lane = lax.broadcasted_iota(jnp.int32, (third, LANES), 1)
        low = pltpu.roll(x[:third], LANES - nf, 1)
        high = pltpu.roll(x[third:lp], LANES - (nf - half), 1)
        return jnp.concatenate([x[:lp], jnp.where(lane < half, low, high)], axis=0)

    def beside(phase, z, first, count):
        lane = lax.broadcasted_iota(jnp.int32, (count, LANES), 1)
        left, right = (yhalo[phase, side, pl.ds(first, count), :] for side in range(2))
        if z:
            left = pltpu.roll(left, LANES - EDGE * z, 1)
        if z != 1:
            right = pltpu.roll(right, (EDGE - EDGE * z) % LANES, 1)
        side = jnp.where(lane < EDGE, left, jnp.where(lane < 2 * EDGE, right, 0.0))
        high = side.astype(BF).astype(F32)
        low = side - high
        return (high + pltpu.roll(low, 2 * EDGE, 1) + pltpu.roll(high, 4 * EDGE, 1)).astype(BF)

    def along_y(rows, sides):
        count = len(rows)
        hi, lo = split(jnp.concatenate([jnp.concatenate(r, axis=0) for r in rows], axis=0))
        side = jnp.concatenate([jnp.concatenate(r, axis=0) for r in sides], axis=0)
        x1 = dot(jnp.concatenate([hi, lo], axis=1), tab("fya")) + dot(
            jnp.concatenate([hi, side], axis=1), tab("fyb")
        )
        n = x1.shape[0] // count
        stacked = [
            jnp.concatenate([x1[k * n : (k + 1) * n, :LANES], x1[k * n : (k + 1) * n, LANES:]], 0)
            for k in range(count)
        ]
        return [split(jnp.concatenate(stacked[k : k + 2], axis=1)) for k in range(0, count, 2)]

    def forward(phase, field, planes):
        spectra = along_y(
            [[field[z]] for z in planes], [[beside(phase, z, EDGE, nx)] for z in planes]
        )
        for q, (hi, lo) in enumerate(spectra):
            x2 = dot(tab("fxa"), jnp.concatenate([hi, lo], axis=0)) + dot(tab("fxb"), hi)
            for k in range(2):
                z = planes[2 * q + k]
                part = x2[:, k * LANES : (k + 1) * LANES]
                mix[z] = part

    def forward_edges(phase, planes):
        spectra = along_y(
            [[xhalo[phase, side, z] for side in range(2)] for z in planes],
            [[beside(phase, z, first, EDGE) for first in (0, EDGE + nx)] for z in planes],
        )
        for q, (hi, lo) in enumerate(spectra):
            x2 = dot(tab("fxh"), jnp.concatenate([hi, lo, hi], axis=0))
            for k in range(2):
                z = planes[2 * q + k]
                part = mix[z] + x2[:, k * LANES : (k + 1) * LANES]
                own[phase, z, pl.ds(0, lp), :] = fold(part[:lx])
                own[phase, z, pl.ds(lp, lp), :] = fold(part[lx:])

    def mix_planes(source, phase, base, conj, add, taken):
        @pl.loop(0, lp // 8, unroll=2)
        def _(s):
            re = pl.ds(pl.multiple_of(s * 8, 8), 8)
            im = pl.ds(pl.multiple_of(lp + s * 8, 8), 8)
            vr = {j: source[phase, j, re, :] for j in taken}
            vi = {j: source[phase, j, im, :] for j in taken}
            kr, ki = {}, {}
            for d in sorted({j - i if conj else i - j for i in range(nz) for j in taken}):
                kr[d] = k2[base + d, re, :]
                ki[d] = k2[base + d, im, :]
            ks = {d: kr[d] - ki[d] if conj else kr[d] + ki[d] for d in kr}
            vs = {j: vr[j] + vi[j] for j in taken}
            for i in range(nz):
                a = b = c = None
                for j in taken:
                    d = j - i if conj else i - j
                    rr, ii, ss = kr[d] * vr[j], ki[d] * vi[j], ks[d] * vs[j]
                    a = rr if a is None else a + rr
                    b = ii if b is None else b + ii
                    c = ss if c is None else c + ss
                yr = a + b if conj else a - b
                yi = c - a + b if conj else c - a - b
                mix[i, re, :] = mix[i, re, :] + yr if add else yr
                mix[i, im, :] = mix[i, im, :] + yi if add else yi

    segments = (((0, EDGE), (nx - EDGE, EDGE)), ((EDGE, nx - 2 * EDGE),))

    def unfolded(z):
        return jnp.concatenate([unfold(mix[z, pl.ds(0, lp)]), unfold(mix[z, pl.ds(lp, lp)])], 0)

    def inverse(planes, parts, write, keep=False, kept=False):
        counts = [sum(count for _, count in segments[p]) for p in parts]
        offset = 2 * sum(count for _, count in segments[0]) * parts[0]
        rows = []
        for z in planes[::2]:
            if kept:
                hi, lo = parts_of[z // 2, 0], parts_of[z // 2, 1]
            else:
                hi, lo = split(jnp.concatenate([unfolded(z), unfolded(z + 1)], axis=1))
            if keep:
                parts_of[z // 2, 0] = hi
                parts_of[z // 2, 1] = lo
            high = tab("ix2", offset, 2 * sum(counts))
            g = dot(high, hi) + dot(tab("ix2", 2 * nx + offset, 2 * sum(counts)), hi) + dot(high, lo)
            for k in range(2):
                part = g[:, k * LANES : (k + 1) * LANES]
                for count in counts:
                    rows.append(jnp.concatenate([part[:count], part[count : 2 * count]], axis=1))
                    part = part[2 * count :]
        hi, lo = split(jnp.concatenate(rows, axis=0))
        both = dot(hi, tab("iy2"))
        values = both[:, :ny] + both[:, ny:] + dot(lo, tab("iy1"))
        row = 0
        for z in planes:
            for p in parts:
                for first, count in segments[p]:
                    write(z, pl.ds(first, count), values[row : row + count])
                    row += count

    def prepare(first):
        block = psf_pad[pl.ds(first, GROUP)].reshape(GROUP * wide, LANES)
        high = block.astype(BF).astype(F32)
        low = block - high
        x1 = dot(
            (high + pltpu.roll(low, wide, 1) + pltpu.roll(high, 2 * wide, 1)).astype(BF),
            tab("ky3"),
        )
        hi, lo = split(x1)
        hi = hi.reshape(GROUP, wide, 2 * LANES)
        lo = lo.reshape(GROUP, wide, 2 * LANES)
        for h in range(GROUP // 2):
            columns = []
            for n in (2 * h, 2 * h + 1):
                parts = []
                for part in (hi[n], lo[n], hi[n]):
                    parts.append(part[:, :LANES])
                    parts.append(part[:, LANES:])
                columns.append(jnp.concatenate(parts, axis=0))
            spectrum = dot(tab("kx3"), jnp.concatenate(columns, axis=1))
            for n in range(2):
                part = spectrum[:, n * LANES : (n + 1) * LANES]
                k2[first + 2 * h + n, pl.ds(0, lp), :] = fold(part[:lx])
                k2[first + 2 * h + n, pl.ds(lp, lp), :] = fold(part[lx:])

    def convolve(phase, field, conj, invert):
        with NS(f"wait_haloy{phase}"):
            settle(hy.at[phase], along_x=False)
        with NS(f"forward{phase}"):
            for z in range(0, nz, 8):
                forward(phase, field, range(z, z + 8))
        if phase == 0:
            with NS("prepare2"):
                prepare(3 * GROUP * gz)
        with NS(f"wait_halox{phase}"):
            settle(hx.at[phase], along_y=False)
        with NS(f"edges{phase}"):
            forward_edges(phase, range(nz))
            for n in range(CHUNKS):
                swap_copy(phase, n).start()
        sign = 1 - 2 * gz if conj else 2 * gz - 1
        with NS(f"mixown{phase}"):
            mix_planes(own, phase, middle, conj, False, range(nz))
        for n in range(CHUNKS):
            with NS(f"waitswap{phase}_{n}"):
                swap_copy(phase, n).wait_recv()
            with NS(f"mixpeer{phase}_{n}"):
                taken = range(n * nz // CHUNKS, (n + 1) * nz // CHUNKS)
                mix_planes(peer, phase, middle + sign * nz, conj, True, taken)
        invert()

    with NS("zero"):
        zero_missing(0)
        zero_missing(1)
    with NS("wait_est"):
        load_est.wait()
    with NS("pack0"):
        do_pack(0, est_ref, pl.ds(0, nx))
    with NS("barrier"):
        if close:
            pl.semaphore_wait(barrier, beside_x + beside_y + beside_x * beside_y + 1)
        else:
            pl.semaphore_wait(barrier, everyone - 1)
    with NS("send0"):
        send_halo(0, est_ref, SIDES_Y)
        send_halo(0, est_ref, CORNERS)
        send_halo(0, est_ref, SIDES_X, pl.ds(0, nz))

    with NS("wait_loads"):
        load_index.wait()
        load_psf.wait()
        load_table.wait()
        load_view.wait()
    with NS("psf_prep"):
        chosen = psf[index_ref[0]]
        total = jnp.sum(chosen, axis=0)
        total = jnp.sum(jnp.sum(total, axis=1, keepdims=True), axis=0, keepdims=True)
        psf_pad[...] = jnp.zeros(psf_pad.shape, F32)
        psf_pad[pl.ds(0, extent), pl.ds(0, extent), pl.ds(0, extent)] = (
            chosen * (1.0 / total)[None]
        )

    with NS("prepare1"):

        @pl.loop(1, 3)
        def _(g):
            prepare(g * GROUP)

    def write_ratio(z, rows, blurred):
        ratio[z, rows, :] = view_ref[z, rows, :] / blurred

    def invert_blurred():
        for first, count in STEPS:
            with NS(f"inverse0_{first}"):
                inverse(range(first, first + count), (0,), write_ratio, keep=True)
                if first + count == nz:
                    for start, rows in segments[0]:
                        do_pack(1, ratio, pl.ds(start, rows))
                    send_halo(1, ratio, CORNERS)

                @pl.when(gz == 0)
                def _():
                    send_halo(1, ratio, SIDES_X, pl.ds(first, count))

                if first:

                    @pl.when(gz == 1)
                    def _():
                        send_halo(1, ratio, SIDES_X, pl.ds(0, first))

        with NS("inverse0_middle"):
            inverse(range(nz), (1,), write_ratio, kept=True)
            @pl.when(gz == 1)
            def _():
                send_halo(1, ratio, SIDES_X, pl.ds(*STEPS[-1]))

            for start, rows in segments[1]:
                do_pack(1, ratio, pl.ds(start, rows))
            send_halo(1, ratio, SIDES_Y)

    convolve(0, est_ref, False, invert_blurred)

    with NS("prepare3"):
        prepare(3 * GROUP * (1 - gz))
        cols5 = four_ref.shape[2] // 2
        i = lax.broadcasted_iota(jnp.int32, (LANES, LANES), 0)
        j = lax.broadcasted_iota(jnp.int32, (LANES, LANES), 1)
        target = i // (ny // cols5) + gy * cols5
        place5[...] = jnp.where(j == target, 1.0 / (nz * 2 * 32 * 32), 0.0).astype(BF)

    def write_update(z, rows, correction):
        out_ref[z, rows, :] = est_ref[z, rows, :] * correction

    def invert_correction():
        with NS("inverse1"):
            inverse(range(nz), (0, 1), write_update)

    convolve(1, ratio, True, invert_correction)

    with NS("five_send"):
        rows5 = four_ref.shape[1] // 2
        total = out_ref[0]
        for z in range(1, nz):
            total = total + out_ref[z]
        summed = jnp.sum(total.reshape(rows5, nx // rows5, ny), axis=1)
        hi, lo = split(summed)
        mine[...] = dot(hi, place5[...]) + dot(lo, place5[...])

        def slot(x, y, z):
            return (x * gyn + y) * 2 + z

        def send_tile(device):
            pltpu.make_async_remote_copy(
                src_ref=mine,
                dst_ref=tiles.at[slot(gx, gy, gz)],
                send_sem=gs,
                recv_sem=gr,
                device_id=device,
                device_id_type=MESH,
            ).start()

        for_others(send_tile)
        tiles[slot(gx, gy, gz)] = mine[...]

    def pooled(plane):
        hi, lo = split(plane)
        t = dot(hi, tab("py")) + dot(lo, tab("py"))
        hi, lo = split(t)
        return dot(tab("px"), hi) + dot(tab("px"), lo)

    with NS("pyramid"):
        halves = [(out_ref[2 * i] + out_ref[2 * i + 1]) * 0.5 for i in range(nz // 2)]
        quarters = [(halves[2 * i] + halves[2 * i + 1]) * 0.5 for i in range(nz // 4)]
        eighth = (quarters[0] + quarters[1]) * 0.5
        r4, c4 = places[3][0], places[3][2]
        last = pooled(eighth)
        share[0] = last[r4 : r4 + 8]
        share_copy = pltpu.make_async_remote_copy(
            src_ref=share.at[0], dst_ref=share_in, send_sem=ps, recv_sem=pr,
            device_id=partner, device_id_type=MESH,
        )
        share_copy.start()
        row, rows, col, cols = places[2]
        three_ref[0] = last[row : row + rows, col : col + cols]
        row, rows, col, cols = places[1]
        for i, plane in enumerate(quarters):
            two_ref[i] = pooled(plane)[row : row + rows, col : col + cols]
        row, rows, col, cols = places[0]
        for i, plane in enumerate(halves):
            one_ref[i] = pooled(plane)[row : row + rows, col : col + cols]
    with NS("share"):
        share_copy.wait()
        both = (share[0] + share_in[...]) * 0.5
        four_ref[0] = both[: places[3][1], c4 : c4 + places[3][3]]
    with NS("settle"):
        for phase in range(2):
            settle(hs.at[phase])
            pltpu.make_async_copy(own.at[phase], peer.at[phase], es.at[phase]).wait()
    with NS("wait_tiles"):
        others = tiles.at[pl.ds(0, everyone - 1)]
        pltpu.make_async_copy(others, others, gs).wait()
        pltpu.make_async_copy(others, others, gr).wait()
    with NS("five"):
        for x in range(gxn):
            five = tiles[slot(x, 0, 0)]
            for n in range(1, 2 * gyn):
                five = five + tiles[slot(x, 0, 0) + n]
            five_ref[0, pl.ds(x * rows5, rows5), :] = five[:, : five_ref.shape[2]]


def write_out(*refs):
    sems = refs[12]
    copies = [pltpu.make_async_copy(refs[i], refs[6 + i], sems.at[i]) for i in range(6)]
    for copy in copies:
        copy.start()
    for copy in copies:
        copy.wait()


def local(sizes, estimate, view_data, psf_stack, view_index):
    gxn, gyn = sizes
    nz, nx, ny = estimate.shape
    extent = psf_stack.shape[1]
    table, where, places = tables(nx, ny, extent)
    lx = nx + 2 * EDGE
    lp = 2 * (lx // 3)
    wide = extent + 1
    everyone = 2 * gxn * gyn
    vmem = pl.BlockSpec(memory_space=pltpu.VMEM)
    hbm = pl.BlockSpec(memory_space=pltpu.HBM)
    rows5, cols5 = nx // 32, ny // 32
    dma = pltpu.SemaphoreType.DMA
    shapes = (
        (nz, nx, ny),
        (nz // 2, nx // 2, ny // 2),
        (nz // 4, nx // 4, ny // 4),
        (nz // 8, nx // 8, ny // 8),
        (1, nx // 16, ny // 16),
        (1, rows5 * gxn, cols5 * gyn),
    )
    results = pl.pallas_call(
        functools.partial(kernel, sizes, where, places),
        out_shape=tuple(pltpu.VMEM(s, F32) for s in shapes),
        in_specs=[hbm] * 5,
        out_specs=(vmem,) * 6,
        scratch_shapes=[
            pltpu.SMEM(view_index.shape, view_index.dtype),
            pltpu.VMEM(estimate.shape, F32),
            pltpu.VMEM(view_data.shape, F32),
            pltpu.VMEM(psf_stack.shape, F32),
            pltpu.VMEM(table.shape, BF),
            pltpu.VMEM((wide, wide, LANES), F32),
            pltpu.VMEM((wide, 2 * lp, LANES), F32),
            pltpu.VMEM((2, nz, 2 * lp, LANES), F32),
            pltpu.VMEM((2, nz, 2 * lp, LANES), F32),
            pltpu.VMEM((nz, 2 * lx, LANES), F32),
            pltpu.VMEM((nz // 2, 2, 2 * lx, 2 * LANES), BF),
            pltpu.VMEM((nz, nx, ny), F32),
            pltpu.VMEM((2, 2, nx, LANES), F32),
            pltpu.VMEM((2, 2, nz, EDGE, ny), F32),
            pltpu.VMEM((2, 2, lx, LANES), F32),
            pltpu.VMEM((1, 8, LANES), F32),
            pltpu.VMEM((8, LANES), F32),
            pltpu.VMEM((LANES, LANES), BF),
            pltpu.VMEM((rows5, LANES), F32),
            pltpu.VMEM((everyone, rows5, LANES), F32),
            pltpu.VMEM((2 * nz * EDGE + 2 * nx + 4 * EDGE, LANES), F32),
            dma((5,)),
            dma((2,)),
            dma((2,)),
            dma((2,)),
            dma((2,)),
            dma((2, CHUNKS)),
            dma,
            dma,
            dma,
            dma,
        ],
        compiler_params=pltpu.CompilerParams(
            collective_id=0, has_side_effects=True, vmem_limit_bytes=48 * 1024 * 1024
        ),
        name="deconvolve",
    )(
        view_index,
        *[
            pltpu.with_memory_space_constraint(a, pltpu.HBM)
            for a in (estimate, view_data, psf_stack, jnp.asarray(table))
        ],
    )
    return pl.pallas_call(
        write_out,
        out_shape=tuple(jax.ShapeDtypeStruct(s, F32) for s in shapes),
        in_specs=[vmem] * 6,
        out_specs=(hbm,) * 6,
        scratch_shapes=[dma((6,))],
        name="write_out",
    )(*[pltpu.with_memory_space_constraint(r, pltpu.VMEM) for r in results])


def solution(mesh):
    return jax.shard_map(
        functools.partial(local, (mesh.shape["gx"], mesh.shape["gy"])),
        mesh=mesh,
        in_specs=(P("gz", "gx", "gy"), P("gz", "gx", "gy"), P(), P()),
        out_specs=(
            P("gz", "gx", "gy"),
            P("gz", "gx", "gy"),
            P("gz", "gx", "gy"),
            P("gz", "gx", "gy"),
            P(None, "gx", "gy"),
            P(),
        ),
        check_vma=False,
    )
```
